32 devices in a mesh: rep: 1 (over z), dp: 32 (over x, y, core).
Axes of the slice: x: 4, y: 4, z: 1, core: 2. Of those that a mesh axis runs over, the one named last changes fastest.
The devices are a block of a 4x4x8 slice.
Arguments:
- x: bfloat16 [32, 1024, 512], P(('rep', 'dp'))
- dy: bfloat16 [32, 1024, 512], P(('rep', 'dp'))
- w_gate: bfloat16 [2, 512, 8192], replicated
- w_up: bfloat16 [2, 512, 8192], replicated
- w_down: bfloat16 [2, 8192, 512], replicated
- m_w_gate: float32 [2, 512, 8192], P(None, 'dp')
- m_w_up: float32 [2, 512, 8192], P(None, 'dp')
- m_w_down: float32 [2, 8192, 512], P(None, 'dp')
- v_w_gate: float32 [2, 512, 8192], P(None, 'dp')
- v_w_up: float32 [2, 512, 8192], P(None, 'dp')
- v_w_down: float32 [2, 8192, 512], P(None, 'dp')
Outputs:
- output 1: bfloat16 [2, 512, 8192], P('rep')
- output 2: bfloat16 [2, 512, 8192], P('rep')
- output 3: bfloat16 [2, 8192, 512], P('rep')
- output 4: float32 [2, 512, 8192], P('rep', 'dp')
- output 5: float32 [2, 512, 8192], P('rep', 'dp')
- output 6: float32 [2, 8192, 512], P('rep', 'dp')
- output 7: float32 [2, 512, 8192], P('rep', 'dp')
- output 8: float32 [2, 512, 8192], P('rep', 'dp')
- output 9: float32 [2, 8192, 512], P('rep', 'dp')
All inputs are finite; a program needn't handle non-finite values.
Results may differ from the reference program's by a relative error of at most 0.022.
Values are sent between devices in bfloat16 or wider.
A program may use at most 768 MiB of HBM per device.

```python
import jax
import jax.numpy as jnp
from jax import lax

SEQUENCES = 32
TOKENS = 1024
D = 512
FF = 8192
LAYERS = 2
NAMES = ("w_gate", "w_up", "w_down")
SHAPES = {"w_gate": (LAYERS, D, FF), "w_up": (LAYERS, D, FF), "w_down": (LAYERS, FF, D)}


def bump(key, n, height):
    away = (jnp.arange(n, dtype=jnp.int32) - jax.random.randint(key, (), 0, n, jnp.int32)) % n
    return jnp.where(away < n // 8, height, 1.0)


def together(key, own, strength):
    shared = jax.random.normal(key, own.shape[1:], jnp.float32)
    return (own + strength * shared) * lax.rsqrt(1 + strength * strength)


def setup_inputs(seed: int = 0, part: int = 0) -> dict:
    kx, kdy, ka, kb, kz, kf, kh, kl, *keys = jax.random.split(jax.random.key(seed), 8 + 3 * len(NAMES))
    kx, kdy, ka, kb = (jax.random.fold_in(k, part) for k in (kx, kdy, ka, kb))
    kw, km, kv = (keys[i::3] for i in range(3))
    shape = (SEQUENCES, TOKENS, D)
    much_x, much_dy = jax.random.uniform(kz, (2,), jnp.float32, 0.0, 1.0)
    loud = 2.0 ** jax.random.uniform(jax.random.fold_in(kz, 1), (), jnp.float32, -1.0, 2.0)
    layers = 2.0 ** jax.random.uniform(kl, (LAYERS, 1, 1), jnp.float32, -1.0, 1.0)
    x = together(ka, jax.random.normal(kx, shape, jnp.float32), much_x) * bump(kf, D, 4.0)
    dy = together(kb, jax.random.normal(kdy, shape, jnp.float32), much_dy)
    drawn = {"x": x.astype(jnp.bfloat16), "dy": (loud * dy * (SEQUENCES * TOKENS) ** -0.5).astype(jnp.bfloat16)}
    for key, name in zip(kw, NAMES, strict=True):
        w = jax.random.normal(key, SHAPES[name], jnp.float32) * SHAPES[name][1] ** -0.5
        drawn[name] = (w * {"w_gate": 1.0, "w_up": bump(kh, FF, 4.0), "w_down": layers}[name]).astype(jnp.bfloat16)
    for key, name in zip(km, NAMES, strict=True):
        drawn[f"m_{name}"] = 0.1 * jax.random.normal(key, SHAPES[name], jnp.float32)
    for key, name in zip(kv, NAMES, strict=True):
        drawn[f"v_{name}"] = jax.random.uniform(key, SHAPES[name], jnp.float32, 0.005, 0.015)
    return drawn


def matmul(a, w):
    return jnp.dot(a, w, preferred_element_type=jnp.float32).astype(jnp.bfloat16)


def normed(h):
    wide = h.astype(jnp.float32)
    scale = lax.rsqrt(jnp.mean(wide**2, -1, keepdims=True) + 1e-6)
    return (wide * scale).astype(jnp.bfloat16)


def layer(h, w):
    a = normed(h)
    gate = jnp.dot(a, w["w_gate"], preferred_element_type=jnp.float32)
    up = jnp.dot(a, w["w_up"], preferred_element_type=jnp.float32)
    return h + matmul((jax.nn.silu(gate) * up).astype(jnp.bfloat16), w["w_down"])


def adamw(w, m, v, g):
    m = 0.9 * m + 0.1 * g
    v = 0.95 * v + 0.05 * g * g
    step = m * lax.rsqrt(v + 1e-8) + 0.1 * w
    return (w - 0.02 * step).astype(jnp.bfloat16), m, v


def clipped(gradients, sum_of_squares, count):
    factor = jnp.minimum(1.0, 0.5 * lax.rsqrt(sum_of_squares / count + 1e-30))
    return [g * factor for g in gradients]


def stack(weights, h):
    return lax.scan(lambda h, w: (layer(h, w), None), h, weights)[0]


def reference(x, dy, w_gate, w_up, w_down, m_w_gate, m_w_up, m_w_down, v_w_gate, v_w_up, v_w_down):
    weights = dict(zip(NAMES, (w_gate, w_up, w_down), strict=True))

    def take(so_far, sequence):
        h, by_y = sequence
        _, back = jax.vjp(lambda w: stack(w, h), weights)
        return jax.tree.map(lambda total, term: total + term.astype(jnp.float32), so_far, back(by_y)[0]), None

    none_yet = {name: jnp.zeros(w.shape, jnp.float32) for name, w in weights.items()}
    by_weights, _ = lax.scan(take, none_yet, (x, dy))
    gradients = [by_weights[name].astype(jnp.bfloat16).astype(jnp.float32) for name in NAMES]
    gradients = clipped(gradients, sum(jnp.sum(g * g) for g in gradients), sum(g.size for g in gradients))
    new = [
        adamw(w.astype(jnp.float32), m, v, g)
        for w, m, v, g in zip((w_gate, w_up, w_down), (m_w_gate, m_w_up, m_w_down), (v_w_gate, v_w_up, v_w_down), gradients, strict=True)
    ]
    return tuple(one[which] for which in range(3) for one in new)
```

```python
import functools

import jax
import jax.numpy as jnp
from jax import lax
from jax.experimental import pallas as pl
from jax.experimental.pallas import tpu as pltpu
from jax.sharding import PartitionSpec as P

F32, BF16 = jnp.float32, jnp.bfloat16
MESH = pl.DeviceIdType.MESH
NT = (((1,), (1,)), ((), ()))
CHUNK = 512
PIECE = 2048
VMEM_LIMIT = 60 * 2**20


def dot(a, b):
    return jnp.dot(a, b, preferred_element_type=F32)


def dot_nt(a, b):
    return lax.dot_general(a, b, NT, preferred_element_type=F32)


def scale_of(wide):
    return lax.rsqrt(jnp.mean(wide * wide, -1, keepdims=True) + 1e-6)


def forward_kernel(steps, x_ref, wg_ref, wu_ref, wd_ref, h_ref, a_ref, acc_ref):
    f = pl.program_id(0)

    @pl.when(f == 0)
    def _():
        wide = x_ref[...].astype(F32)
        a_ref[...] = (wide * scale_of(wide)).astype(BF16)
        acc_ref[...] = jnp.zeros_like(acc_ref)

    a = a_ref[...]
    gate, up = dot(a, wg_ref[0]), dot(a, wu_ref[0])
    act = (gate * jax.nn.sigmoid(gate) * up).astype(BF16)
    acc_ref[...] += dot(act, wd_ref[0])

    @pl.when(f == steps - 1)
    def _():
        h_ref[...] = x_ref[...] + acc_ref[...].astype(BF16)


def forward(x, wg, wu, wd, number):
    (tokens, d), ff = x.shape, wg.shape[2]
    steps = ff // CHUNK
    whole = pl.BlockSpec((tokens, d), lambda f: (0, 0))
    return pl.pallas_call(
        functools.partial(forward_kernel, steps),
        name="layer_forward",
        grid=(steps,),
        out_shape=jax.ShapeDtypeStruct(x.shape, BF16),
        in_specs=[whole]
        + [pl.BlockSpec((1, d, CHUNK), lambda f: (number, 0, f))] * 2
        + [pl.BlockSpec((1, CHUNK, d), lambda f: (number, f, 0))],
        out_specs=whole,
        scratch_shapes=[pltpu.VMEM((tokens, d), BF16), pltpu.VMEM((tokens, d), F32)],
        compiler_params=pltpu.CompilerParams(vmem_limit_bytes=VMEM_LIMIT),
        cost_estimate=pl.CostEstimate(flops=6 * tokens * d * ff, bytes_accessed=6 * d * ff, transcendentals=0),
    )(x, wg, wu, wd)


def backward_kernel(steps, inner, h_ref, dy_ref, wg_ref, wu_ref, wd_ref, ggu_ref, gd_ref, *rest):
    if inner:
        dh_ref, a_ref, at_ref, dg_acc, du_acc = rest
    else:
        a_ref, at_ref = rest
    f = pl.program_id(0)

    @pl.when(f == 0)
    def _():
        wide = h_ref[...].astype(F32)
        a = (wide * scale_of(wide)).astype(BF16)
        a_ref[...] = a
        at_ref[...] = a.T
        if inner:
            dg_acc[...] = jnp.zeros_like(dg_acc)
            du_acc[...] = jnp.zeros_like(du_acc)

    a, dy = a_ref[...], dy_ref[...]
    gate, up = dot(a, wg_ref[0]), dot(a, wu_ref[0])
    dact = dot_nt(dy, wd_ref[0]).astype(BF16).astype(F32)
    sig = jax.nn.sigmoid(gate)
    silu = gate * sig
    act = (silu * up).astype(BF16)
    dup = (dact * silu).astype(BF16)
    dgate = (dact * up * (sig + silu * (1.0 - sig))).astype(BF16)
    if inner:
        dg_acc[...] += dot_nt(dgate, wg_ref[0])
        du_acc[...] += dot_nt(dup, wu_ref[0])
    at = at_ref[...]
    ggu_ref[0] = dot(at, dgate).astype(BF16).reshape(ggu_ref.shape[1:])
    ggu_ref[1] = dot(at, dup).astype(BF16).reshape(ggu_ref.shape[1:])
    dwd = lax.dot_general(act, dy, (((0,), (0,)), ((), ())), preferred_element_type=F32).astype(BF16)
    blocks, rows, columns = gd_ref.shape
    d = dwd.shape[1]
    for b in range(blocks):
        for k in range(columns // d):
            at_row = (b * (columns // d) + k) * rows
            gd_ref[b, :, k * d : (k + 1) * d] = dwd[at_row : at_row + rows]

    if inner:

        @pl.when(f == steps - 1)
        def _():
            da = (dg_acc[...].astype(BF16).astype(F32) + du_acc[...].astype(BF16).astype(F32)).astype(BF16).astype(F32)
            wide = h_ref[...].astype(F32)
            s = scale_of(wide)
            dot_ = jnp.mean(da * wide, -1, keepdims=True)
            dh = (da * s - wide * (s * s * s * dot_)).astype(BF16)
            dh_ref[...] = dy_ref[...] + dh


def backward(h, dy, wg, wu, wd, number, devices, inner):
    (tokens, d), ff = h.shape, wg.shape[2]
    steps, rows = ff // CHUNK, d // devices
    share = ff // devices
    whole = pl.BlockSpec((tokens, d), lambda f: (0, 0))
    outs = [jax.ShapeDtypeStruct((2, devices, rows, ff), BF16), jax.ShapeDtypeStruct((devices, rows, ff), BF16)]
    out_specs = [
        pl.BlockSpec((2, devices, rows, CHUNK), lambda f: (0, 0, 0, f)),
        pl.BlockSpec((CHUNK // share, rows, ff), lambda f: (f, 0, 0)),
    ]
    scratch = [pltpu.VMEM((tokens, d), BF16), pltpu.VMEM((d, tokens), BF16)]
    if inner:
        outs.append(jax.ShapeDtypeStruct((tokens, d), BF16))
        out_specs.append(whole)
        scratch += [pltpu.VMEM((tokens, d), F32)] * 2
    return pl.pallas_call(
        functools.partial(backward_kernel, steps, inner),
        name="layer_backward_inner" if inner else "layer_backward_first",
        grid=(steps,),
        out_shape=outs,
        in_specs=[whole, whole]
        + [pl.BlockSpec((1, d, CHUNK), lambda f: (number, 0, f))] * 2
        + [pl.BlockSpec((1, CHUNK, d), lambda f: (number, f, 0))],
        out_specs=out_specs,
        scratch_shapes=scratch,
        compiler_params=pltpu.CompilerParams(vmem_limit_bytes=VMEM_LIMIT),
        cost_estimate=pl.CostEstimate(
            flops=(16 if inner else 12) * tokens * d * ff, bytes_accessed=12 * d * ff, transcendentals=0
        ),
    )(h, dy, wg, wu, wd)


def wide_sum(*terms):
    total = terms[0].astype(F32)
    for t in terms[1:]:
        total = total + t.astype(F32)
    return total


def reduce_kernel(side, per_unit, g_refs, out_ref, sq_ref, S, r0, r1, r2, R, r3, r4, sqs, sqr,
                  load_sem, s0, v0, s1, v1, s2, v2, s3, v3, s4, v4, qs, qv):
    me = lax.axis_index("dp")
    core, chip = lax.rem(me, 2), lax.div(me, 2)
    y, x = lax.rem(chip, side), lax.div(chip, side)
    at = (x, y)

    def device(x, y, c):
        return {"dp": (x * side + y) * 2 + c}

    def step(axis, by):
        moved = lax.rem(at[axis] + by + side, side)
        return device(moved, y, core) if axis == 0 else device(x, moved, core)

    partner = device(x, y, 1 - core)
    neighbour = [[step(axis, 1), step(axis, -1)] for axis in (0, 1)]
    up = [lax.rem(at[axis] + 1, side) for axis in (0, 1)]
    down = [lax.rem(at[axis] + side - 1, side) for axis in (0, 1)]
    across = [lax.rem(at[axis] + 2, side) for axis in (0, 1)]
    piece = S.shape[-1]
    half = piece // 2
    quarter = half // 2
    units = out_ref.shape[0]
    N = units * per_unit

    barrier = pltpu.get_barrier_semaphore()
    for other in [partner] + neighbour[0] + neighbour[1]:
        pl.semaphore_signal(barrier, inc=1, device_id=other, device_id_type=MESH)
    pl.semaphore_wait(barrier, 5)

    def s_at(st, slot, p, lo=0, n=4):
        if st == 0:
            return S.at[slot, p, pl.ds(lo, n), :, pl.ds(0, half)]
        return S.at[slot, pl.ds(lo, n), p, :, pl.ds(half, half)]

    def remote(src, dst, ssem, rsem, to):
        return pltpu.make_async_remote_copy(
            src_ref=src, dst_ref=dst, send_sem=ssem, recv_sem=rsem, device_id=to, device_id_type=MESH
        )

    def columns(i):
        return pl.ds(pl.multiple_of(lax.rem(i, per_unit) * piece, piece), piece)

    def g_at(ref, index, i, c):
        if index is None:
            return ref.at[:, :, c, :, columns(i)]
        return ref.at[index, :, :, c, :, columns(i)]

    def load(ref, index, i, slot, par):
        return pltpu.make_async_copy(g_at(ref, index, i, core), S.at[slot], load_sem.at[par])

    def send0(ref, index, i, par):
        return remote(g_at(ref, index, i, 1 - core), r0.at[par], s0.at[par], v0.at[par], partner)

    def send1(st, d, slot, par):
        return remote(
            s_at(st, slot, across[st], 2 * d, 2), r1.at[par, st, d], s1.at[par, st, d], v1.at[par, st, d], neighbour[st][d]
        )

    def send2(st, d, slot, par):
        to = up[st] if d == 0 else down[st]
        return remote(s_at(st, slot, to), r2.at[par, st, d], s2.at[par, st, d], v2.at[par, st, d], neighbour[st][d])

    def send3(st, d, slot, par):
        o = 1 - st
        src = R.at[slot, st, across[o], :, pl.ds(d * quarter, quarter)]
        return remote(src, r3.at[par, st, d], s3.at[par, st, d], v3.at[par, st, d], neighbour[o][d])

    def send4(st, d, slot, par):
        o = 1 - st
        src = R.at[slot, st, up[o] if d == 0 else down[o]]
        return remote(src, r4.at[par, st, d], s4.at[par, st, d], v4.at[par, st, d], neighbour[o][d])

    BOTH = [(st, d) for st in (0, 1) for d in (0, 1)]
    sqs[0] = jnp.zeros(sqs.shape[1:], F32)

    def active(i):
        return jnp.logical_and(i >= 0, i < N)

    def body(t, carry):
        now, before = lax.rem(t, 2), lax.rem(t + 1, 2)

        def slot4(i):
            return lax.rem(i + 8, 4)

        i5 = t - 5

        @pl.when(active(i5))
        def _():
            slot = slot4(i5)
            for st in (0, 1):
                for d in (0, 1):
                    send4(st, d, slot, before).wait_recv()
                o = 1 - st
                total = wide_sum(R[slot, st, at[o]], r4[before, st, 0], r4[before, st, 1]).astype(BF16)
                where = pl.ds(pl.multiple_of(lax.rem(i5, per_unit) * piece + st * half, half), half)
                out_ref[lax.div(i5, per_unit), :, where] = total
                wide = total.astype(F32)
                square = (wide * wide).reshape(2, 8, half // 128, 128)
                sqs[0] += jnp.sum(jnp.sum(square, axis=2), axis=0)

        i4 = t - 4

        @pl.when(active(i4 - 2))
        def _():
            for st, d in BOTH:
                send4(st, d, slot4(i4 - 2), now).wait_send()

        @pl.when(active(i4))
        def _():
            slot = slot4(i4)
            for st, d in BOTH:
                send3(st, d, slot, before).wait_recv()
                o = 1 - st
                to, part = (up[o] if d == 0 else down[o]), pl.ds(d * quarter, quarter)
                R[slot, st, to, :, part] = wide_sum(R[slot, st, to, :, part], r3[before, st, d]).astype(BF16)
            for st, d in BOTH:
                send4(st, d, slot, now).start()

        i3 = t - 3

        @pl.when(active(i3 - 2))
        def _():
            for st, d in BOTH:
                send3(st, d, slot4(i3 - 2), now).wait_send()

        @pl.when(active(i3))
        def _():
            slot = slot4(i3)
            for st, d in BOTH:
                send2(st, d, slot, before).wait_recv()
            for st in (0, 1):
                for k in range(side):
                    mine = S[slot, at[0], k, :, :half] if st == 0 else S[slot, k, at[1], :, half:]
                    R[slot, st, k] = wide_sum(mine, r2[before, st, 0, k], r2[before, st, 1, k]).astype(BF16)
            for st, d in BOTH:
                send3(st, d, slot, now).start()

        i2 = t - 2

        @pl.when(active(i2 - 2))
        def _():
            for st, d in BOTH:
                send2(st, d, slot4(i2 - 2), now).wait_send()

        @pl.when(active(i2))
        def _():
            slot = slot4(i2)
            for st, d in BOTH:
                send1(st, d, slot, before).wait_recv()
                to = up[st] if d == 0 else down[st]
                for k in (2 * d, 2 * d + 1):
                    if st == 0:
                        S[slot, to, k, :, :half] = wide_sum(S[slot, to, k, :, :half], r1[before, st, d, k - 2 * d]).astype(BF16)
                    else:
                        S[slot, k, to, :, half:] = wide_sum(S[slot, k, to, :, half:], r1[before, st, d, k - 2 * d]).astype(BF16)
            for st, d in BOTH:
                send2(st, d, slot, now).start()

        i1 = t - 1

        @pl.when(active(i1 - 2))
        def _():
            for st, d in BOTH:
                send1(st, d, slot4(i1 - 2), now).wait_send()

        @pl.when(active(i1))
        def _():
            slot = slot4(i1)
            load(g_refs[1], None, i1, slot, before).wait()
            send0(g_refs[1], None, i1, before).wait_recv()

            def add(k, carry):
                kx, ky = lax.div(k, side), lax.rem(k, side)
                S[slot, kx, ky] = wide_sum(S[slot, kx, ky], r0[before, kx, ky]).astype(BF16)
                return carry

            lax.fori_loop(0, side * side, add, 0)
            for st, d in BOTH:
                send1(st, d, slot, now).start()

        @pl.when(active(t - 2))
        def _():
            send0(g_refs[1], None, t - 2, now).wait_send()

        for n, ref in enumerate(g_refs):
            first = 3 * (n // 2) + 2 * (n % 2)
            last = first + 2 - n % 2

            @pl.when(jnp.logical_and(t >= first * per_unit, t < last * per_unit))
            def _(ref=ref, first=first, n=n):
                index = lax.div(t, per_unit) - first if n % 2 == 0 else None
                load(ref, index, t, slot4(t), now).start()
                send0(ref, index, t, now).start()

        return carry

    lax.fori_loop(0, N + 6, body, 0)

    swaps = [partner]
    for axis in (0, 1):
        p = at[axis]
        for q in (p + 1 - 2 * lax.rem(p, 2), side - 1 - p):
            swaps.append(device(q, y, core) if axis == 0 else device(x, q, core))
    for n, other in enumerate(swaps):
        swap = remote(sqs.at[n], sqr.at[n], qs.at[n], qv.at[n], other)
        swap.start()
        swap.wait()
        sqs[n + 1] = sqs[n] + sqr[n]
    sq_ref[...] = sqs[len(swaps)]


def reduce_scatter(gradients, n):
    side = round((n // 2) ** 0.5)
    assert side == 4 and n == 2 * side * side
    rows, ff = gradients[0].shape[2:]
    flat = [
        g.reshape(2, side, side, 2, rows, ff) if g.ndim == 4 else g.reshape(side, side, 2, rows, ff) for g in gradients
    ]
    units = 3 * (len(flat) // 2)
    half = PIECE // 2
    dma = pltpu.SemaphoreType.DMA

    def kernel(*refs):
        reduce_kernel(side, ff // PIECE, refs[: len(flat)], *refs[len(flat) :])

    vmem = pl.BlockSpec(memory_space=pltpu.VMEM)
    return pl.pallas_call(
        kernel,
        name="reduce_gradients",
        out_shape=(jax.ShapeDtypeStruct((units, rows, ff), BF16), jax.ShapeDtypeStruct((8, 128), F32)),
        in_specs=[pl.BlockSpec(memory_space=pl.ANY)] * len(flat),
        out_specs=(vmem, vmem),
        scratch_shapes=[
            pltpu.VMEM((4, side, side, rows, PIECE), BF16),
            pltpu.VMEM((2, side, side, rows, PIECE), BF16),
            pltpu.VMEM((2, 2, 2, 2, rows, half), BF16),
            pltpu.VMEM((2, 2, 2, side, rows, half), BF16),
            pltpu.VMEM((4, 2, side, rows, half), BF16),
            pltpu.VMEM((2, 2, 2, rows, half // 2), BF16),
            pltpu.VMEM((2, 2, 2, rows, half), BF16),
            pltpu.VMEM((6, 8, 128), F32),
            pltpu.VMEM((5, 8, 128), F32),
            dma((2,)),
            dma((2,)),
            dma((2,)),
        ]
        + [dma((2, 2, 2))] * 8
        + [dma((5,))] * 2,
        compiler_params=pltpu.CompilerParams(collective_id=1, has_side_effects=True, vmem_limit_bytes=40 * 2**20),
        cost_estimate=pl.CostEstimate(flops=10**9, bytes_accessed=10**8, transcendentals=0),
    )(*flat)


def adamw(w, m, v, g):
    m = 0.9 * m + 0.1 * g
    v = 0.95 * v + 0.05 * g * g
    step = m * lax.rsqrt(v + 1e-8) + 0.1 * w
    return (w - 0.02 * step).astype(jnp.bfloat16), m, v


def solution(mesh):
    n = mesh.shape["dp"]

    def step(x, dy, *arrays):
        w, m, v = (arrays[i : i + 3] for i in (0, 3, 6))
        x, dy = x[0], dy[0]
        me = lax.axis_index("dp")
        h = forward(x, *w, 0)
        gu1, d1, dh = backward(h, dy, *w, 1, n, True)
        gu0, d0 = backward(x, dh, *w, 0, n, False)
        summed, squares = reduce_scatter([gu1, d1, gu0, d0], n)
        count = sum(t.size for t in w)
        factor = jnp.minimum(1.0, 0.5 * lax.rsqrt(jnp.sum(squares) / count + 1e-30))
        outs = []
        for k in range(3):
            rows = m[k].shape[1]
            g = jnp.stack([summed[3 + k], summed[k]])
            if k == 2:
                g = g.reshape(2, g.shape[1], -1, m[k].shape[2]).swapaxes(1, 2).reshape(m[k].shape)
            own = lax.dynamic_slice_in_dim(w[k], me * rows, rows, 1)
            outs.append(adamw(own.astype(F32), m[k], v[k], g.astype(F32) * factor))
        new = [lax.all_gather(one[0], "dp", axis=1, tiled=True) for one in outs]
        return (*new, *(one[1] for one in outs), *(one[2] for one in outs))

    seq, rep, own = P(("rep", "dp"), None, None), P(None, None, None), P(None, "dp", None)
    return jax.shard_map(
        step,
        mesh=mesh,
        in_specs=(seq, seq) + (rep,) * 3 + (own,) * 6,
        out_specs=(P("rep", None, None),) * 3 + (P("rep", "dp", None),) * 6,
        check_vma=False,
    )
```

```python
import functools

import jax
import jax.numpy as jnp
from jax import lax
from jax.experimental import pallas as pl
from jax.experimental.pallas import tpu as pltpu
from jax.sharding import PartitionSpec as P

F32, BF16 = jnp.float32, jnp.bfloat16
MESH = pl.DeviceIdType.MESH
NT = (((1,), (1,)), ((), ()))
CHUNK = 512
VMEM_LIMIT = 60 * 2**20
GATHER_QUARTERS = 16


def dot(a, b):
    return jnp.dot(a, b, preferred_element_type=F32)


def dot_nt(a, b):
    return lax.dot_general(a, b, NT, preferred_element_type=F32)


def scale_of(wide):
    return lax.rsqrt(jnp.mean(wide * wide, -1, keepdims=True) + 1e-6)


def forward_kernel(steps, x_ref, wg_ref, wu_ref, wd_ref, h_ref, a_ref, acc_ref):
    f = pl.program_id(0)

    @pl.when(f == 0)
    def _():
        wide = x_ref[...].astype(F32)
        a_ref[...] = (wide * scale_of(wide)).astype(BF16)
        acc_ref[...] = jnp.zeros_like(acc_ref)

    a = a_ref[...]
    gate, up = dot(a, wg_ref[0]), dot(a, wu_ref[0])
    act = (gate * jax.nn.sigmoid(gate) * up).astype(BF16)
    acc_ref[...] += dot(act, wd_ref[0])

    @pl.when(f == steps - 1)
    def _():
        h_ref[...] = x_ref[...] + acc_ref[...].astype(BF16)


def forward(x, wg, wu, wd, number):
    (tokens, d), ff = x.shape, wg.shape[2]
    steps = ff // CHUNK
    whole = pl.BlockSpec((tokens, d), lambda f: (0, 0))
    return pl.pallas_call(
        functools.partial(forward_kernel, steps),
        name="layer_forward",
        grid=(steps,),
        out_shape=jax.ShapeDtypeStruct(x.shape, BF16),
        in_specs=[whole]
        + [pl.BlockSpec((1, d, CHUNK), lambda f: (number, 0, f))] * 2
        + [pl.BlockSpec((1, CHUNK, d), lambda f: (number, f, 0))],
        out_specs=whole,
        scratch_shapes=[pltpu.VMEM((tokens, d), BF16), pltpu.VMEM((tokens, d), F32)],
        compiler_params=pltpu.CompilerParams(vmem_limit_bytes=VMEM_LIMIT),
        cost_estimate=pl.CostEstimate(flops=6 * tokens * d * ff, bytes_accessed=6 * d * ff, transcendentals=0),
    )(x, wg, wu, wd)


def wide_sum(*terms):
    total = terms[0].astype(F32)
    for t in terms[1:]:
        total = total + t.astype(F32)
    return total


def remote(src, dst, ssem, rsem, to):
    return pltpu.make_async_remote_copy(
        src_ref=src, dst_ref=dst, send_sem=ssem, recv_sem=rsem, device_id=to, device_id_type=MESH
    )


class Torus:
    def __init__(self, side):
        me = lax.axis_index("dp")
        self.side = side
        self.core, chip = lax.rem(me, 2), lax.div(me, 2)
        self.at = (lax.div(chip, side), lax.rem(chip, side))
        self.partner = self.device(*self.at, 1 - self.core)
        self.up = [lax.rem(p + 1, side) for p in self.at]
        self.down = [lax.rem(p + side - 1, side) for p in self.at]
        self.across = [lax.rem(p + 2, side) for p in self.at]
        self.neighbour = [[self.along(axis, p[axis]) for p in (self.up, self.down)] for axis in (0, 1)]

    def device(self, x, y, c):
        return {"dp": (x * self.side + y) * 2 + c}

    def along(self, axis, p):
        return self.device(p, self.at[1], self.core) if axis == 0 else self.device(self.at[0], p, self.core)

    def next(self, axis, d):
        return self.up[axis] if d == 0 else self.down[axis]

    def greet(self):
        barrier = pltpu.get_barrier_semaphore()
        for other in [self.partner] + self.neighbour[0] + self.neighbour[1]:
            pl.semaphore_signal(barrier, inc=1, device_id=other, device_id_type=MESH)
        pl.semaphore_wait(barrier, 5)


BOTH = [(st, d) for st in (0, 1) for d in (0, 1)]


class Pipe:
    def __init__(self, torus, count, lag, sources, sink, scratch):
        self.torus, self.count, self.lag, self.sources, self.sink = torus, count, lag, sources, sink
        self.S, self.r0, self.r1, self.r2, self.R, self.r3, self.r4, self.s0, self.v0, *rest = scratch
        (self.s1, self.v1, self.s2, self.v2, self.s3, self.v3, self.s4, self.v4) = rest
        self.half = self.S.shape[-1] // 2

    @staticmethod
    def scratch(side, rows, width):
        half, dma = width // 2, pltpu.SemaphoreType.DMA
        return [
            pltpu.VMEM((4, side, side, rows, width), BF16),
            pltpu.VMEM((2, side, side, rows, width), BF16),
            pltpu.VMEM((2, 2, 2, 2, rows, half), BF16),
            pltpu.VMEM((2, 2, 2, side, rows, half), BF16),
            pltpu.VMEM((4, 2, side, rows, half), BF16),
            pltpu.VMEM((2, 2, 2, rows, half // 2), BF16),
            pltpu.VMEM((2, 2, 2, rows, half), BF16),
            dma((2,)),
            dma((2,)),
        ] + [dma((2, 2, 2))] * 8

    def s_at(self, st, slot, p, lo=0, n=4):
        if st == 0:
            return self.S.at[slot, p, pl.ds(lo, n), :, pl.ds(0, self.half)]
        return self.S.at[slot, pl.ds(lo, n), p, :, pl.ds(self.half, self.half)]

    def send0(self, view, par):
        return remote(view, self.r0.at[par], self.s0.at[par], self.v0.at[par], self.torus.partner)

    def any0(self, par):
        return self.send0(self.S.at[0], par)

    def send1(self, st, d, slot, par):
        src, k = self.s_at(st, slot, self.torus.across[st], 2 * d, 2), (par, st, d)
        return remote(src, self.r1.at[k], self.s1.at[k], self.v1.at[k], self.torus.neighbour[st][d])

    def send2(self, st, d, slot, par):
        src, k = self.s_at(st, slot, self.torus.next(st, d)), (par, st, d)
        return remote(src, self.r2.at[k], self.s2.at[k], self.v2.at[k], self.torus.neighbour[st][d])

    def send3(self, st, d, slot, par):
        o, k, quarter = 1 - st, (par, st, d), self.half // 2
        src = self.R.at[slot, st, self.torus.across[o], :, pl.ds(d * quarter, quarter)]
        return remote(src, self.r3.at[k], self.s3.at[k], self.v3.at[k], self.torus.neighbour[o][d])

    def send4(self, st, d, slot, par):
        o, k = 1 - st, (par, st, d)
        src = self.R.at[slot, st, self.torus.next(o, d)]
        return remote(src, self.r4.at[k], self.s4.at[k], self.v4.at[k], self.torus.neighbour[o][d])

    def active(self, i):
        return jnp.logical_and(i >= 0, i < self.count)

    def within(self, i, source):
        return jnp.logical_and(i >= source[0], i < source[1])

    def sent(self, i, send, now):
        @pl.when(self.active(i))
        def _():
            for st, d in BOTH:
                send(st, d, lax.rem(i + 8, 4), now).wait_send()

    def turn(self, t):
        torus, S, R, half = self.torus, self.S, self.R, self.half
        now, before = lax.rem(t, 2), lax.rem(t + 1, 2)
        i = t - self.lag

        def slot4(i):
            return lax.rem(i + 8, 4)

        @pl.when(self.active(i - 5))
        def _():
            slot = slot4(i - 5)
            for st in (0, 1):
                for d in (0, 1):
                    self.send4(st, d, slot, before).wait_recv()
                total = wide_sum(R[slot, st, torus.at[1 - st]], self.r4[before, st, 0], self.r4[before, st, 1])
                self.sink(i - 5, st, total.astype(BF16))

        self.sent(i - 6, self.send4, now)

        @pl.when(self.active(i - 4))
        def _():
            slot, quarter = slot4(i - 4), half // 2
            for st, d in BOTH:
                self.send3(st, d, slot, before).wait_recv()
                to, part = torus.next(1 - st, d), pl.ds(d * quarter, quarter)
                R[slot, st, to, :, part] = wide_sum(R[slot, st, to, :, part], self.r3[before, st, d]).astype(BF16)
            for st, d in BOTH:
                self.send4(st, d, slot, now).start()

        self.sent(i - 5, self.send3, now)

        @pl.when(self.active(i - 3))
        def _():
            slot = slot4(i - 3)
            for st, d in BOTH:
                self.send2(st, d, slot, before).wait_recv()
            for st in (0, 1):
                for k in range(torus.side):
                    mine = S[slot, torus.at[0], k, :, :half] if st == 0 else S[slot, k, torus.at[1], :, half:]
                    R[slot, st, k] = wide_sum(mine, self.r2[before, st, 0, k], self.r2[before, st, 1, k]).astype(BF16)
            for st, d in BOTH:
                self.send3(st, d, slot, now).start()

        self.sent(i - 4, self.send2, now)

        @pl.when(self.active(i - 2))
        def _():
            slot = slot4(i - 2)
            for st, d in BOTH:
                self.send1(st, d, slot, before).wait_recv()
                to = torus.next(st, d)
                for k in (0, 1):
                    arrived = self.r1[before, st, d, k]
                    if st == 0:
                        S[slot, to, 2 * d + k, :, :half] = wide_sum(S[slot, to, 2 * d + k, :, :half], arrived).astype(BF16)
                    else:
                        S[slot, 2 * d + k, to, :, half:] = wide_sum(S[slot, 2 * d + k, to, :, half:], arrived).astype(BF16)
            for st, d in BOTH:
                self.send2(st, d, slot, now).start()

        self.sent(i - 3, self.send1, now)

        @pl.when(self.active(i - 1))
        def _():
            self.any0(before).wait_recv()
            slot = slot4(i - 1)
            for source in self.sources:

                @pl.when(self.within(i - 1, source))
                def _(source=source):
                    def add(k, carry):
                        kx, ky = lax.div(k, torus.side), lax.rem(k, torus.side)
                        mine = source[2](i - 1, torus.core).at[kx, ky][...]
                        S[slot, kx, ky] = wide_sum(mine, self.r0[before, kx, ky]).astype(BF16)
                        return carry

                    lax.fori_loop(0, torus.side**2, add, 0)

            for st, d in BOTH:
                self.send1(st, d, slot, now).start()

        @pl.when(self.active(i - 2))
        def _():
            self.any0(now).wait_send()

        for source in self.sources:

            @pl.when(self.within(i, source))
            def _(source=source):
                self.send0(source[2](i, 1 - torus.core), now).start()


def gradient_kernel(
    side, ff, chunk, x_ref, h_ref, dy_ref, wg_hbm, wu_hbm, wd_hbm, out_ref, sq_ref,
    a_ref, at_ref, dy_now, dg_acc, du_acc, w_buf, w_sem, C, D, sqs, sqr, qs, qv, *pipes,
):
    torus = Torus(side)
    steps = ff // chunk
    rows, d = out_ref.shape[1], x_ref.shape[1]
    torus.greet()

    def set_input(ref):
        wide = ref[...].astype(F32)
        a = (wide * scale_of(wide)).astype(BF16)
        a_ref[...] = a
        at_ref[...] = a.T

    def loads(t, slot):
        number, f = 1 - lax.div(t, steps), lax.rem(t, steps)
        part = pl.ds(pl.multiple_of(f * chunk, chunk), chunk)
        return [
            pltpu.make_async_copy(wg_hbm.at[number, :, part], w_buf.at[slot, 0], w_sem.at[slot, 0]),
            pltpu.make_async_copy(wu_hbm.at[number, :, part], w_buf.at[slot, 1], w_sem.at[slot, 1]),
            pltpu.make_async_copy(wd_hbm.at[number, part, :], w_buf.at[slot, 2], w_sem.at[slot, 2]),
        ]

    for copy in loads(0, 0):
        copy.start()
    dy_now[...] = dy_ref[...]
    sqs[0] = jnp.zeros(sqs.shape[1:], F32)
    dg_acc[...] = jnp.zeros_like(dg_acc)
    du_acc[...] = jnp.zeros_like(du_acc)
    set_input(h_ref)

    def compute(t, inner):
        slot, c_slot = lax.rem(t, 2), lax.rem(t, C.shape[0])
        f = lax.rem(t, steps)
        a, dy = a_ref[...], dy_now[...]
        wg, wu, wd = (w_buf[slot, k] for k in range(3))
        gate, up = dot(a, wg), dot(a, wu)
        dact = dot_nt(dy, wd).astype(BF16).astype(F32)
        sig = jax.nn.sigmoid(gate)
        silu = gate * sig
        act = (silu * up).astype(BF16)
        dup = (dact * silu).astype(BF16)
        dgate = (dact * up * (sig + silu * (1.0 - sig))).astype(BF16)
        if inner:
            dg_acc[...] += dot_nt(dgate, wg)
            du_acc[...] += dot_nt(dup, wu)
        at = at_ref[...]
        C[c_slot, ..., :chunk] = dot(at, dgate).astype(BF16).reshape(side, side, 2, rows, chunk)
        C[c_slot, ..., chunk:] = dot(at, dup).astype(BF16).reshape(side, side, 2, rows, chunk)
        dwd = lax.dot_general(act, dy, (((0,), (0,)), ((), ())), preferred_element_type=F32).astype(BF16)
        pieces = ff // d
        for b in range(2):
            for k in range(pieces):
                row = (b * pieces + k) * rows
                D[1 if inner else 0, lax.div(f, side), lax.rem(f, side), b, :, k * d : (k + 1) * d] = dwd[row : row + rows]

    def squares(total):
        wide = total.astype(F32)
        sqs[0] += jnp.sum(jnp.sum((wide * wide).reshape(2, 8, -1, 128), axis=2), axis=0)

    def d_view(layer, first, width):
        def view(i, c):
            return D.at[layer, :, :, c, :, pl.ds(pl.multiple_of((i - first) * width, width), width)]

        return view

    def c_view(i, c):
        return C.at[lax.rem(i, C.shape[0]), :, :, c]

    def sink_main(i, st, total):
        squares(total)

        @pl.when(i < 2 * steps)
        def _():
            where = pl.ds(pl.multiple_of(lax.rem(i, steps) * chunk, chunk), chunk)
            out_ref[3 * lax.div(i, steps) + st, :, where] = total

        @pl.when(i >= 2 * steps)
        def _():
            where = pl.ds(pl.multiple_of((i - 2 * steps) * 2 * chunk + st * chunk, chunk), chunk)
            out_ref[5, :, where] = total

    def sink_down(i, st, total):
        squares(total)
        width = chunk // 2
        out_ref[2, :, pl.ds(pl.multiple_of(i * chunk + st * width, width), width)] = total

    tail = steps // 2
    n = len(pipes) // 2
    main = Pipe(
        torus, 2 * steps + tail, 1,
        [(0, 2 * steps, c_view), (2 * steps, 2 * steps + tail, d_view(0, 2 * steps, 2 * chunk))], sink_main, pipes[:n],
    )
    down = Pipe(torus, steps, steps + 1, [(0, steps, d_view(1, 0, chunk))], sink_down, pipes[n:])

    def body(t, carry):
        @pl.when(t == steps)
        def _():
            set_input(x_ref)

        main.turn(t)
        down.turn(t)

        @pl.when(t < 2 * steps)
        def _():
            @pl.when(t + 1 < 2 * steps)
            def _():
                for copy in loads(t + 1, lax.rem(t + 1, 2)):
                    copy.start()

            for copy in loads(t, lax.rem(t, 2)):
                copy.wait()

        @pl.when(t < steps)
        def _():
            compute(t, True)

        @pl.when(t == steps - 1)
        def _():
            da = (dg_acc[...].astype(BF16).astype(F32) + du_acc[...].astype(BF16).astype(F32)).astype(BF16).astype(F32)
            wide = h_ref[...].astype(F32)
            s = scale_of(wide)
            along = jnp.mean(da * wide, -1, keepdims=True)
            dy_now[...] = dy_ref[...] + (da * s - wide * (s * s * s * along)).astype(BF16)

        @pl.when(jnp.logical_and(t >= steps, t < 2 * steps))
        def _():
            compute(t, False)

        return carry

    lax.fori_loop(0, 2 * steps + tail + 7, body, 0)

    swaps = [torus.partner]
    for axis in (0, 1):
        p = torus.at[axis]
        for q in (p + 1 - 2 * lax.rem(p, 2), side - 1 - p):
            swaps.append(torus.along(axis, q))
    for k, other in enumerate(swaps):
        swap = remote(sqs.at[k], sqr.at[k], qs.at[k], qv.at[k], other)
        swap.start()
        swap.wait()
        sqs[k + 1] = sqs[k] + sqr[k]
    sq_ref[...] = sqs[len(swaps)]


def summed_gradients(x, h, dy, w, n):
    (tokens, d), ff = x.shape, w[0].shape[2]
    side = round((n // 2) ** 0.5)
    assert side == 4 and n == 2 * side * side and w[0].shape[0] == 2
    rows, chunk = d // n, CHUNK
    assert 2 * ff // n == chunk
    dma, vmem = pltpu.SemaphoreType.DMA, pl.BlockSpec(memory_space=pltpu.VMEM)
    return pl.pallas_call(
        functools.partial(gradient_kernel, side, ff, chunk),
        name="summed_gradients",
        out_shape=(jax.ShapeDtypeStruct((6, rows, ff), BF16), jax.ShapeDtypeStruct((8, 128), F32)),
        in_specs=[vmem] * 3 + [pl.BlockSpec(memory_space=pl.ANY)] * 3,
        out_specs=(vmem, vmem),
        scratch_shapes=[
            pltpu.VMEM((tokens, d), BF16),
            pltpu.VMEM((d, tokens), BF16),
            pltpu.VMEM((tokens, d), BF16),
            pltpu.VMEM((tokens, d), F32),
            pltpu.VMEM((tokens, d), F32),
            pltpu.VMEM((2, 3, d, chunk), BF16),
            dma((2, 3)),
            pltpu.VMEM((3, side, side, 2, rows, 2 * chunk), BF16),
            pltpu.VMEM((2, side, side, 2, rows, ff), BF16),
            pltpu.VMEM((6, 8, 128), F32),
            pltpu.VMEM((5, 8, 128), F32),
            dma((5,)),
            dma((5,)),
        ]
        + Pipe.scratch(side, rows, 2 * chunk)
        + Pipe.scratch(side, rows, chunk),
        compiler_params=pltpu.CompilerParams(collective_id=1, has_side_effects=True, vmem_limit_bytes=67043328),
        cost_estimate=pl.CostEstimate(flops=28 * tokens * d * ff, bytes_accessed=12 * d * ff, transcendentals=0),
    )(x, h, dy, *w)


def gather_kernel(
    side, own_gate, own_up, own_down, out_gate, out_up, out_down, own_sem, sa, va, sb, vb, sc, vc, sd, vd, se, ve
):
    torus = Torus(side)
    outs, owns = (out_gate, out_up, out_down), (own_gate, own_up, own_down)
    x, y = torus.at
    core = torus.core
    quarter = [ref.shape[-1] // GATHER_QUARTERS for ref in outs[:2]] + [out_down.shape[-2] // GATHER_QUARTERS]
    per_layer = GATHER_QUARTERS // 4
    layers = out_gate.shape[0]
    per_kind = layers * per_layer
    count = 3 * per_kind

    own_copies = [
        pltpu.make_async_copy(own, out.at[:, x, y, core], own_sem.at[k]) for k, (own, out) in enumerate(zip(owns, outs))
    ]
    for copy in own_copies:
        copy.start()
    torus.greet()
    for copy in own_copies:
        copy.wait()

    def part(kind, i, first, n):
        where = pl.ds(
            pl.multiple_of((lax.rem(i, per_layer) * 4 + first) * quarter[kind], quarter[kind]), n * quarter[kind]
        )
        return (slice(None), where) if kind < 2 else (where, slice(None))

    def layer_of(kind, i):
        return lax.div(i - kind * per_kind, per_layer)

    def place(kind, i, st, p, q, first, n):
        where = (p, q) if st == 0 else (q, p)
        return outs[kind].at[(layer_of(kind, i), *where, core, *part(kind, i, first, n))]

    ALL = slice(None)

    def send(src, dst, ss, vs, to):
        return remote(src, dst, ss, vs, to)

    def send_a(kind, i, st, d, par):
        dst = place(kind, i, st, torus.at[st], torus.at[1 - st], 2 * st, 2)
        src = owns[kind].at[(layer_of(kind, i), *part(kind, i, 2 * st, 2))]
        k = (par, st, d)
        return remote(src, dst, sa.at[k], va.at[k], torus.neighbour[1 - st][d])

    def send_b(kind, i, st, d, par):
        o = 1 - st
        ref, k = place(kind, i, st, torus.at[st], torus.next(o, 1 - d), 2 * st + d, 1), (par, st, d)
        return remote(ref, ref, sb.at[k], vb.at[k], torus.neighbour[o][d])

    def send_c(kind, i, st, d, par):
        ref, k = place(kind, i, st, torus.at[st], ALL, 2 * st, 2), (par, st, d)
        return remote(ref, ref, sc.at[k], vc.at[k], torus.neighbour[st][d])

    def send_d(kind, i, st, d, par):
        ref, k = place(kind, i, st, torus.next(st, 1 - d), pl.ds(2 * d, 2), 2 * st, 2), (par, st, d)
        return remote(ref, ref, sd.at[k], vd.at[k], torus.neighbour[st][d])

    def send_e(kind, i, par):
        ref = outs[kind].at[(layer_of(kind, i), ALL, ALL, core, *part(kind, i, 0, 4))]
        return remote(ref, ref, se.at[par], ve.at[par], torus.partner)

    def active(i):
        return jnp.logical_and(i >= 0, i < count)

    sends = [send_a, send_b, send_c, send_d]

    def body(t, carry):
        now, before = lax.rem(t, 2), lax.rem(t + 1, 2)

        @pl.when(active(t - 5))
        def _():
            send_e(0, 0, before).wait_recv()

        @pl.when(active(t - 6))
        def _():
            send_e(0, 0, now).wait_send()

        @pl.when(active(t - 4))
        def _():
            for st, d in BOTH:
                send_d(0, 0, st, d, before).wait_recv()
            for kind in range(3):

                @pl.when(lax.div(t - 4, per_kind) == kind)
                def _(kind=kind):
                    send_e(kind, t - 4, now).start()

        for s in (3, 2, 1, 0):

            @pl.when(active(t - s - 2))
            def _(s=s):
                for st, d in BOTH:
                    sends[s](0, 0, st, d, now).wait_send()

            @pl.when(active(t - s))
            def _(s=s):
                if s:
                    for st, d in BOTH:
                        sends[s - 1](0, 0, st, d, before).wait_recv()
                for kind in range(3):

                    @pl.when(lax.div(t - s, per_kind) == kind)
                    def _(kind=kind):
                        for st, d in BOTH:
                            sends[s](kind, t - s, st, d, now).start()

        return carry

    lax.fori_loop(0, count + 6, body, 0)


def gathered(blocks, n):
    side = round((n // 2) ** 0.5)
    assert side == 4 and n == 2 * side * side
    dma = pltpu.SemaphoreType.DMA
    whole = pl.pallas_call(
        functools.partial(gather_kernel, side),
        name="gather_weights",
        out_shape=[jax.ShapeDtypeStruct((b.shape[0], side, side, 2, *b.shape[1:]), b.dtype) for b in blocks],
        in_specs=[pl.BlockSpec(memory_space=pltpu.VMEM)] * 3,
        out_specs=[pl.BlockSpec(memory_space=pl.ANY)] * 3,
        scratch_shapes=[dma((3,))] + [dma((2, 2, 2))] * 8 + [dma((2,))] * 2,
        compiler_params=pltpu.CompilerParams(collective_id=2, has_side_effects=True, vmem_limit_bytes=16 * 2**20),
        cost_estimate=pl.CostEstimate(flops=10**8, bytes_accessed=10**8, transcendentals=0),
    )(*blocks)
    return [t.reshape(t.shape[0], -1, t.shape[-1]) for t in whole]


def adamw(w, m, v, g):
    m = 0.9 * m + 0.1 * g
    v = 0.95 * v + 0.05 * g * g
    step = m * lax.rsqrt(v + 1e-8) + 0.1 * w
    return (w - 0.02 * step).astype(jnp.bfloat16), m, v


def solution(mesh):
    n = mesh.shape["dp"]

    def step(x, dy, *arrays):
        w, m, v = (arrays[i : i + 3] for i in (0, 3, 6))
        x, dy = x[0], dy[0]
        me = lax.axis_index("dp")
        h = forward(x, *w, 0)
        summed, squares = summed_gradients(x, h, dy, w, n)
        count = sum(t.size for t in w)
        factor = jnp.minimum(1.0, 0.5 * lax.rsqrt(jnp.sum(squares) / count + 1e-30))
        outs = []
        for k in range(3):
            rows = m[k].shape[1]
            g = jnp.stack([summed[3 + k], summed[k]])
            if k == 2:
                g = g.reshape(2, g.shape[1], -1, m[k].shape[2]).swapaxes(1, 2).reshape(m[k].shape)
            own = lax.dynamic_slice_in_dim(w[k], me * rows, rows, 1)
            outs.append(adamw(own.astype(F32), m[k], v[k], g.astype(F32) * factor))
        new = gathered([one[0] for one in outs], n)
        return (*new, *(one[1] for one in outs), *(one[2] for one in outs))

    seq, rep, own = P(("rep", "dp"), None, None), P(None, None, None), P(None, "dp", None)
    return jax.shard_map(
        step,
        mesh=mesh,
        in_specs=(seq, seq) + (rep,) * 3 + (own,) * 6,
        out_specs=(P("rep", None, None),) * 3 + (P("rep", "dp", None),) * 6,
        check_vma=False,
    )
```

```python
import functools

import jax
import jax.numpy as jnp
from jax import lax
from jax.experimental import pallas as pl
from jax.experimental.pallas import tpu as pltpu
from jax.sharding import PartitionSpec as P

F32, BF16 = jnp.float32, jnp.bfloat16
MESH = pl.DeviceIdType.MESH
NT = (((1,), (1,)), ((), ()))
CHUNK = 512
FORWARD_CHUNK = 1024
VMEM_LIMIT = 60 * 2**20
GATHER_QUARTERS = 16


def dot(a, b):
    return jnp.dot(a, b, preferred_element_type=F32)


def dot_nt(a, b):
    return lax.dot_general(a, b, NT, preferred_element_type=F32)


def scale_of(wide):
    return lax.rsqrt(jnp.mean(wide * wide, -1, keepdims=True) + 1e-6)


def forward_kernel(steps, x_ref, wg_ref, wu_ref, wd_ref, h_ref, a_ref, acc_ref):
    f = pl.program_id(0)

    @pl.when(f == 0)
    def _():
        wide = x_ref[...].astype(F32)
        a_ref[...] = (wide * scale_of(wide)).astype(BF16)
        acc_ref[...] = jnp.zeros_like(acc_ref)

    a = a_ref[...]
    gate, up = dot(a, wg_ref[0]), dot(a, wu_ref[0])
    act = (gate * jax.nn.sigmoid(gate) * up).astype(BF16)
    acc_ref[...] += dot(act, wd_ref[0])

    @pl.when(f == steps - 1)
    def _():
        h_ref[...] = x_ref[...] + acc_ref[...].astype(BF16)


def forward(x, wg, wu, wd, number):
    (tokens, d), ff = x.shape, wg.shape[2]
    steps = ff // FORWARD_CHUNK
    whole = pl.BlockSpec((tokens, d), lambda f: (0, 0))
    return pl.pallas_call(
        functools.partial(forward_kernel, steps),
        name="layer_forward",
        grid=(steps,),
        out_shape=jax.ShapeDtypeStruct(x.shape, BF16),
        in_specs=[whole]
        + [pl.BlockSpec((1, d, FORWARD_CHUNK), lambda f: (number, 0, f))] * 2
        + [pl.BlockSpec((1, FORWARD_CHUNK, d), lambda f: (number, f, 0))],
        out_specs=whole,
        scratch_shapes=[pltpu.VMEM((tokens, d), BF16), pltpu.VMEM((tokens, d), F32)],
        compiler_params=pltpu.CompilerParams(vmem_limit_bytes=VMEM_LIMIT),
        cost_estimate=pl.CostEstimate(flops=6 * tokens * d * ff, bytes_accessed=6 * d * ff, transcendentals=0),
    )(x, wg, wu, wd)


def wide_sum(*terms):
    total = terms[0].astype(F32)
    for t in terms[1:]:
        total = total + t.astype(F32)
    return total


def remote(src, dst, ssem, rsem, to):
    return pltpu.make_async_remote_copy(
        src_ref=src, dst_ref=dst, send_sem=ssem, recv_sem=rsem, device_id=to, device_id_type=MESH
    )


class Torus:
    def __init__(self, side):
        me = lax.axis_index("dp")
        self.side = side
        self.core, chip = lax.rem(me, 2), lax.div(me, 2)
        self.at = (lax.div(chip, side), lax.rem(chip, side))
        self.partner = self.device(*self.at, 1 - self.core)
        self.up = [lax.rem(p + 1, side) for p in self.at]
        self.down = [lax.rem(p + side - 1, side) for p in self.at]
        self.across = [lax.rem(p + 2, side) for p in self.at]
        self.neighbour = [[self.along(axis, p[axis]) for p in (self.up, self.down)] for axis in (0, 1)]

    def device(self, x, y, c):
        return {"dp": (x * self.side + y) * 2 + c}

    def along(self, axis, p):
        return self.device(p, self.at[1], self.core) if axis == 0 else self.device(self.at[0], p, self.core)

    def next(self, axis, d):
        return self.up[axis] if d == 0 else self.down[axis]

    def greet(self):
        barrier = pltpu.get_barrier_semaphore()
        for other in [self.partner] + self.neighbour[0] + self.neighbour[1]:
            pl.semaphore_signal(barrier, inc=1, device_id=other, device_id_type=MESH)
        pl.semaphore_wait(barrier, 5)


BOTH = [(st, d) for st in (0, 1) for d in (0, 1)]


class Pipe:
    def __init__(self, torus, count, lag, sources, sink, scratch):
        self.torus, self.count, self.lag, self.sources, self.sink = torus, count, lag, sources, sink
        self.S, self.r0, self.r1, self.r2, self.R, self.r3, self.r4, self.s0, self.v0, *rest = scratch
        (self.s1, self.v1, self.s2, self.v2, self.s3, self.v3, self.s4, self.v4) = rest
        self.half = self.S.shape[-1] // 2

    @staticmethod
    def scratch(side, rows, width):
        half, dma = width // 2, pltpu.SemaphoreType.DMA
        return [
            pltpu.VMEM((6, side, side, rows, width), BF16),
            pltpu.VMEM((4, side, side, rows, width), BF16),
            pltpu.VMEM((4, 2, 2, 2, rows, half), BF16),
            pltpu.VMEM((4, 2, 2, side, rows, half), BF16),
            pltpu.VMEM((6, 2, side, rows, half), BF16),
            pltpu.VMEM((4, 2, 2, rows, half // 2), BF16),
            pltpu.VMEM((4, 2, 2, rows, half), BF16),
            dma((4,)),
            dma((4,)),
        ] + [dma((4,))] * 8

    def s_at(self, st, slot, p, lo=0, n=4):
        if st == 0:
            return self.S.at[slot, p, pl.ds(lo, n), :, pl.ds(0, self.half)]
        return self.S.at[slot, pl.ds(lo, n), p, :, pl.ds(self.half, self.half)]

    def send0(self, view, par):
        return remote(view, self.r0.at[par], self.s0.at[par], self.v0.at[par], self.torus.partner)

    def any0(self, par):
        return self.send0(self.S.at[0], par)

    def send1(self, st, d, slot, par):
        src, k = self.s_at(st, slot, self.torus.across[st], 2 * d, 2), (par, st, d)
        return remote(src, self.r1.at[k], self.s1.at[par], self.v1.at[par], self.torus.neighbour[st][d])

    def send2(self, st, d, slot, par):
        src, k = self.s_at(st, slot, self.torus.next(st, d)), (par, st, d)
        return remote(src, self.r2.at[k], self.s2.at[par], self.v2.at[par], self.torus.neighbour[st][d])

    def send3(self, st, d, slot, par):
        o, k, quarter = 1 - st, (par, st, d), self.half // 2
        src = self.R.at[slot, st, self.torus.across[o], :, pl.ds(d * quarter, quarter)]
        return remote(src, self.r3.at[k], self.s3.at[par], self.v3.at[par], self.torus.neighbour[o][d])

    def send4(self, st, d, slot, par):
        o, k = 1 - st, (par, st, d)
        src = self.R.at[slot, st, self.torus.next(o, d)]
        return remote(src, self.r4.at[k], self.s4.at[par], self.v4.at[par], self.torus.neighbour[o][d])

    def all(self, n, par):
        r, s, v = ((self.r1, self.s1, self.v1), (self.r2, self.s2, self.v2), (self.r3, self.s3, self.v3), (self.r4, self.s4, self.v4))[n - 1]
        return remote(r.at[par], r.at[par], s.at[par], v.at[par], self.torus.partner)

    def active(self, i):
        return jnp.logical_and(i >= 0, i < self.count)

    def within(self, i, source):
        return jnp.logical_and(i >= source[0], i < source[1])

    def sent(self, i, n, now):
        @pl.when(self.active(i))
        def _():
            self.all(n, now).wait_send()

    def turn(self, t):
        torus, S, R, half = self.torus, self.S, self.R, self.half
        now, before = lax.rem(t, 4), lax.rem(t + 2, 4)
        i = t - self.lag

        def slot6(i):
            return lax.rem(i, 6)

        @pl.when(self.active(i - 10))
        def _():
            slot = slot6(i - 10)
            self.all(4, before).wait_recv()
            for st in (0, 1):
                total = wide_sum(R[slot, st, torus.at[1 - st]], self.r4[before, st, 0], self.r4[before, st, 1])
                self.sink(i - 10, st, total.astype(BF16))

        self.sent(i - 12, 4, now)

        @pl.when(self.active(i - 8))
        def _():
            slot, quarter = slot6(i - 8), half // 2
            self.all(3, before).wait_recv()
            for st, d in BOTH:
                to, part = torus.next(1 - st, d), pl.ds(d * quarter, quarter)
                R[slot, st, to, :, part] = wide_sum(R[slot, st, to, :, part], self.r3[before, st, d]).astype(BF16)
            for st, d in BOTH:
                self.send4(st, d, slot, now).start()

        self.sent(i - 10, 3, now)

        @pl.when(self.active(i - 6))
        def _():
            slot = slot6(i - 6)
            self.all(2, before).wait_recv()
            for st in (0, 1):
                for k in range(torus.side):
                    mine = S[slot, torus.at[0], k, :, :half] if st == 0 else S[slot, k, torus.at[1], :, half:]
                    R[slot, st, k] = wide_sum(mine, self.r2[before, st, 0, k], self.r2[before, st, 1, k]).astype(BF16)
            for st, d in BOTH:
                self.send3(st, d, slot, now).start()

        self.sent(i - 8, 2, now)

        @pl.when(self.active(i - 4))
        def _():
            slot = slot6(i - 4)
            self.all(1, before).wait_recv()
            for st, d in BOTH:
                to = torus.next(st, d)
                for k in (0, 1):
                    arrived = self.r1[before, st, d, k]
                    if st == 0:
                        S[slot, to, 2 * d + k, :, :half] = wide_sum(S[slot, to, 2 * d + k, :, :half], arrived).astype(BF16)
                    else:
                        S[slot, 2 * d + k, to, :, half:] = wide_sum(S[slot, 2 * d + k, to, :, half:], arrived).astype(BF16)
            for st, d in BOTH:
                self.send2(st, d, slot, now).start()

        self.sent(i - 6, 1, now)

        @pl.when(self.active(i - 2))
        def _():
            self.any0(before).wait_recv()
            slot = slot6(i - 2)
            for source in self.sources:

                @pl.when(self.within(i - 2, source))
                def _(source=source):
                    def add(k, carry):
                        kx, ky = lax.div(k, torus.side), lax.rem(k, torus.side)
                        mine = source[2](i - 2, torus.core).at[kx, ky][...]
                        S[slot, kx, ky] = wide_sum(mine, self.r0[before, kx, ky]).astype(BF16)
                        return carry

                    lax.fori_loop(0, torus.side**2, add, 0, unroll=4)

            for st, d in BOTH:
                self.send1(st, d, slot, now).start()

        @pl.when(self.active(i - 2))
        def _():
            self.any0(before).wait_send()

        for source in self.sources:

            @pl.when(self.within(i, source))
            def _(source=source):
                self.send0(source[2](i, 1 - torus.core), now).start()


def gradient_kernel(
    side, ff, chunk, count, x_ref, h_ref, dy_ref, wg_hbm, wu_hbm, wd_hbm, out_ref, factor_ref,
    a_ref, at_ref, dy_now, dg_acc, du_acc, w_buf, w_sem, C, D, sqs, sqr, qs, qv, *pipes,
):
    torus = Torus(side)
    steps = ff // chunk
    rows, d = out_ref.shape[1], x_ref.shape[1]
    torus.greet()

    def set_input(ref):
        wide = ref[...].astype(F32)
        a = (wide * scale_of(wide)).astype(BF16)
        a_ref[...] = a
        at_ref[...] = a.T

    def loads(t, slot):
        number, f = 1 - lax.div(t, steps), lax.rem(t, steps)
        part = pl.ds(pl.multiple_of(f * chunk, chunk), chunk)
        return [
            pltpu.make_async_copy(wg_hbm.at[number, :, part], w_buf.at[slot, 0], w_sem.at[slot, 0]),
            pltpu.make_async_copy(wu_hbm.at[number, :, part], w_buf.at[slot, 1], w_sem.at[slot, 1]),
            pltpu.make_async_copy(wd_hbm.at[number, part, :], w_buf.at[slot, 2], w_sem.at[slot, 2]),
        ]

    for copy in loads(0, 0):
        copy.start()
    dy_now[...] = dy_ref[...]
    sqs[0] = jnp.zeros(sqs.shape[1:], F32)
    dg_acc[...] = jnp.zeros_like(dg_acc)
    du_acc[...] = jnp.zeros_like(du_acc)
    set_input(h_ref)

    def compute(t, inner):
        slot, c_slot = lax.rem(t, 2), lax.rem(t, C.shape[0])
        f = lax.rem(t, steps)
        a, dy = a_ref[...], dy_now[...]
        wg, wu, wd = (w_buf[slot, k] for k in range(3))
        gate, up = dot(a, wg), dot(a, wu)
        dact = dot_nt(dy, wd).astype(BF16).astype(F32)
        sig = jax.nn.sigmoid(gate)
        silu = gate * sig
        act = (silu * up).astype(BF16)
        dup = (dact * silu).astype(BF16)
        dgate = (dact * up * (sig + silu * (1.0 - sig))).astype(BF16)
        if inner:
            dg_acc[...] += dot_nt(dgate, wg)
            du_acc[...] += dot_nt(dup, wu)
        at = at_ref[...]
        C[c_slot, ..., :chunk] = dot(at, dgate).astype(BF16).reshape(side, side, 2, rows, chunk)
        C[c_slot, ..., chunk:] = dot(at, dup).astype(BF16).reshape(side, side, 2, rows, chunk)
        dwd = lax.dot_general(act, dy, (((0,), (0,)), ((), ())), preferred_element_type=F32).astype(BF16)
        pieces = ff // d
        for b in range(2):
            for k in range(pieces):
                row = (b * pieces + k) * rows
                D[1 if inner else 0, lax.div(f, side), lax.rem(f, side), b, :, k * d : (k + 1) * d] = dwd[row : row + rows]

    def squares(total):
        wide = total.astype(F32)
        sqs[0] += jnp.sum(jnp.sum((wide * wide).reshape(2, 8, -1, 128), axis=2), axis=0)

    def d_view(layer, first, width):
        def view(i, c):
            return D.at[layer, :, :, c, :, pl.ds(pl.multiple_of((i - first) * width, width), width)]

        return view

    def c_view(i, c):
        return C.at[lax.rem(i, C.shape[0]), :, :, c]

    def sink_main(i, st, total):
        squares(total)

        @pl.when(i < 2 * steps)
        def _():
            where = pl.ds(pl.multiple_of(lax.rem(i, steps) * chunk, chunk), chunk)
            out_ref[3 * lax.div(i, steps) + st, :, where] = total

        @pl.when(i >= 2 * steps)
        def _():
            where = pl.ds(pl.multiple_of((i - 2 * steps) * 2 * chunk + st * chunk, chunk), chunk)
            out_ref[5, :, where] = total

    def sink_down(i, st, total):
        squares(total)
        width = chunk // 2
        out_ref[2, :, pl.ds(pl.multiple_of(i * chunk + st * width, width), width)] = total

    tail = steps // 2
    n = len(pipes) // 2
    main = Pipe(
        torus, 2 * steps + tail, 1,
        [(0, 2 * steps, c_view), (2 * steps, 2 * steps + tail, d_view(0, 2 * steps, 2 * chunk))], sink_main, pipes[:n],
    )
    down = Pipe(torus, steps, steps + 1, [(0, steps, d_view(1, 0, chunk))], sink_down, pipes[n:])

    def body(t, carry):
        @pl.when(t == steps)
        def _():
            set_input(x_ref)

        main.turn(t)
        down.turn(t)

        @pl.when(t < 2 * steps)
        def _():
            @pl.when(t + 1 < 2 * steps)
            def _():
                for copy in loads(t + 1, lax.rem(t + 1, 2)):
                    copy.start()

            for copy in loads(t, lax.rem(t, 2)):
                copy.wait()

        @pl.when(t < steps)
        def _():
            compute(t, True)

        @pl.when(t == steps - 1)
        def _():
            da = (dg_acc[...].astype(BF16).astype(F32) + du_acc[...].astype(BF16).astype(F32)).astype(BF16).astype(F32)
            wide = h_ref[...].astype(F32)
            s = scale_of(wide)
            along = jnp.mean(da * wide, -1, keepdims=True)
            dy_now[...] = dy_ref[...] + (da * s - wide * (s * s * s * along)).astype(BF16)

        @pl.when(jnp.logical_and(t >= steps, t < 2 * steps))
        def _():
            compute(t, False)

        return carry

    lax.fori_loop(0, 2 * steps + tail + 13, body, 0)

    swaps = [torus.partner]
    for axis in (0, 1):
        p = torus.at[axis]
        for q in (p + 1 - 2 * lax.rem(p, 2), side - 1 - p):
            swaps.append(torus.along(axis, q))
    for k, other in enumerate(swaps):
        swap = remote(sqs.at[k], sqr.at[k], qs.at[k], qv.at[k], other)
        swap.start()
        swap.wait()
        sqs[k + 1] = sqs[k] + sqr[k]
    total = jnp.broadcast_to(jnp.sum(sqs[len(swaps)], keepdims=True), factor_ref.shape)
    factor_ref[...] = jnp.minimum(1.0, 0.5 * lax.rsqrt(total / count + 1e-30))


def summed_gradients(x, h, dy, w, n):
    (tokens, d), ff = x.shape, w[0].shape[2]
    side = round((n // 2) ** 0.5)
    assert side == 4 and n == 2 * side * side and w[0].shape[0] == 2
    rows, chunk = d // n, CHUNK
    assert 2 * ff // n == chunk
    dma, vmem = pltpu.SemaphoreType.DMA, pl.BlockSpec(memory_space=pltpu.VMEM)
    return pl.pallas_call(
        functools.partial(gradient_kernel, side, ff, chunk, sum(t.size for t in w)),
        name="summed_gradients",
        out_shape=(jax.ShapeDtypeStruct((6, rows, ff), BF16), jax.ShapeDtypeStruct((8, 128), F32)),
        in_specs=[vmem] * 3 + [pl.BlockSpec(memory_space=pl.ANY)] * 3,
        out_specs=(vmem, vmem),
        scratch_shapes=[
            pltpu.VMEM((tokens, d), BF16),
            pltpu.VMEM((d, tokens), BF16),
            pltpu.VMEM((tokens, d), BF16),
            pltpu.VMEM((tokens, d), F32),
            pltpu.VMEM((tokens, d), F32),
            pltpu.VMEM((2, 3, d, chunk), BF16),
            dma((2, 3)),
            pltpu.VMEM((3, side, side, 2, rows, 2 * chunk), BF16),
            pltpu.VMEM((2, side, side, 2, rows, ff), BF16),
            pltpu.VMEM((6, 8, 128), F32),
            pltpu.VMEM((5, 8, 128), F32),
            dma((5,)),
            dma((5,)),
        ]
        + Pipe.scratch(side, rows, 2 * chunk)
        + Pipe.scratch(side, rows, chunk),
        compiler_params=pltpu.CompilerParams(collective_id=1, has_side_effects=True, vmem_limit_bytes=67043328),
        cost_estimate=pl.CostEstimate(flops=28 * tokens * d * ff, bytes_accessed=12 * d * ff, transcendentals=0),
    )(x, h, dy, *w)


def gather_kernel(
    side, own_gate, own_up, own_down, out_gate, out_up, out_down, own_sem, sa, va, sb, vb, sc, vc, sd, vd, se, ve
):
    torus = Torus(side)
    outs, owns = (out_gate, out_up, out_down), (own_gate, own_up, own_down)
    x, y = torus.at
    core = torus.core
    quarter = [ref.shape[-1] // GATHER_QUARTERS for ref in outs[:2]] + [out_down.shape[-2] // GATHER_QUARTERS]
    per_layer = GATHER_QUARTERS // 4
    layers = out_gate.shape[0]
    per_kind = layers * per_layer
    count = 3 * per_kind

    own_copies = [
        pltpu.make_async_copy(own, out.at[:, x, y, core], own_sem.at[k]) for k, (own, out) in enumerate(zip(owns, outs))
    ]
    for copy in own_copies:
        copy.start()
    torus.greet()
    for copy in own_copies:
        copy.wait()

    def part(kind, i, first, n):
        where = pl.ds(
            pl.multiple_of((lax.rem(i, per_layer) * 4 + first) * quarter[kind], quarter[kind]), n * quarter[kind]
        )
        return (slice(None), where) if kind < 2 else (where, slice(None))

    def layer_of(kind, i):
        return lax.div(i - kind * per_kind, per_layer)

    def place(kind, i, st, p, q, first, n):
        where = (p, q) if st == 0 else (q, p)
        return outs[kind].at[(layer_of(kind, i), *where, core, *part(kind, i, first, n))]

    ALL = slice(None)

    def send_a(kind, i, st, d, par):
        dst = place(kind, i, st, torus.at[st], torus.at[1 - st], 2 * st, 2)
        src = owns[kind].at[(layer_of(kind, i), *part(kind, i, 2 * st, 2))]
        k = (par, st, d)
        return remote(src, dst, sa.at[k], va.at[k], torus.neighbour[1 - st][d])

    def send_b(kind, i, st, d, par):
        o = 1 - st
        ref, k = place(kind, i, st, torus.at[st], torus.next(o, 1 - d), 2 * st + d, 1), (par, st, d)
        return remote(ref, ref, sb.at[k], vb.at[k], torus.neighbour[o][d])

    def send_c(kind, i, st, d, par):
        ref, k = place(kind, i, st, torus.at[st], ALL, 2 * st, 2), (par, st, d)
        return remote(ref, ref, sc.at[k], vc.at[k], torus.neighbour[st][d])

    def send_d(kind, i, st, d, par):
        ref, k = place(kind, i, st, torus.next(st, 1 - d), pl.ds(2 * d, 2), 2 * st, 2), (par, st, d)
        return remote(ref, ref, sd.at[k], vd.at[k], torus.neighbour[st][d])

    def send_e(kind, i, par):
        ref = outs[kind].at[(layer_of(kind, i), ALL, ALL, core, *part(kind, i, 0, 4))]
        return remote(ref, ref, se.at[par], ve.at[par], torus.partner)

    def active(i):
        return jnp.logical_and(i >= 0, i < count)

    sends = [send_a, send_b, send_c, send_d]

    def body(t, carry):
        now, before = lax.rem(t, 4), lax.rem(t + 2, 4)

        @pl.when(active(t - 10))
        def _():
            send_e(0, 0, before).wait_recv()

        @pl.when(active(t - 12))
        def _():
            send_e(0, 0, now).wait_send()

        @pl.when(active(t - 8))
        def _():
            for st, d in BOTH:
                send_d(0, 0, st, d, before).wait_recv()
            for kind in range(3):

                @pl.when(lax.div(t - 8, per_kind) == kind)
                def _(kind=kind):
                    send_e(kind, t - 8, now).start()

        for s in (3, 2, 1, 0):

            @pl.when(active(t - 2 * s - 4))
            def _(s=s):
                for st, d in BOTH:
                    sends[s](0, 0, st, d, now).wait_send()

            @pl.when(active(t - 2 * s))
            def _(s=s):
                if s:
                    for st, d in BOTH:
                        sends[s - 1](0, 0, st, d, before).wait_recv()
                for kind in range(3):

                    @pl.when(lax.div(t - 2 * s, per_kind) == kind)
                    def _(kind=kind):
                        for st, d in BOTH:
                            sends[s](kind, t - 2 * s, st, d, now).start()

        return carry

    lax.fori_loop(0, count + 12, body, 0)


def gathered(blocks, n):
    side = round((n // 2) ** 0.5)
    assert side == 4 and n == 2 * side * side
    dma = pltpu.SemaphoreType.DMA
    whole = pl.pallas_call(
        functools.partial(gather_kernel, side),
        name="gather_weights",
        out_shape=[jax.ShapeDtypeStruct((b.shape[0], side, side, 2, *b.shape[1:]), b.dtype) for b in blocks],
        in_specs=[pl.BlockSpec(memory_space=pltpu.VMEM)] * 3,
        out_specs=[pl.BlockSpec(memory_space=pl.ANY)] * 3,
        scratch_shapes=[dma((3,))] + [dma((4, 2, 2))] * 8 + [dma((4,))] * 2,
        compiler_params=pltpu.CompilerParams(collective_id=2, has_side_effects=True, vmem_limit_bytes=16 * 2**20),
        cost_estimate=pl.CostEstimate(flops=10**8, bytes_accessed=10**8, transcendentals=0),
    )(*blocks)
    return [t.reshape(t.shape[0], -1, t.shape[-1]) for t in whole]


def adamw(w, m, v, g):
    m = 0.9 * m + 0.1 * g
    v = 0.95 * v + 0.05 * g * g
    step = m * lax.rsqrt(v + 1e-8) + 0.1 * w
    return (w - 0.02 * step).astype(jnp.bfloat16), m, v


def solution(mesh):
    n = mesh.shape["dp"]

    def step(x, dy, *arrays):
        w, m, v = (arrays[i : i + 3] for i in (0, 3, 6))
        x, dy = x[0], dy[0]
        me = lax.axis_index("dp")
        h = forward(x, *w, 0)
        summed, factor = summed_gradients(x, h, dy, w, n)
        factor = factor[0, 0]
        outs = []
        for k in range(3):
            rows = m[k].shape[1]
            g = jnp.stack([summed[3 + k], summed[k]])
            if k == 2:
                g = g.reshape(2, g.shape[1], -1, m[k].shape[2]).swapaxes(1, 2).reshape(m[k].shape)
            own = lax.dynamic_slice_in_dim(w[k], me * rows, rows, 1)
            outs.append(adamw(own.astype(F32), m[k], v[k], g.astype(F32) * factor))
        new = gathered([one[0] for one in outs], n)
        return (*new, *(one[1] for one in outs), *(one[2] for one in outs))

    seq, rep, own = P(("rep", "dp"), None, None), P(None, None, None), P(None, "dp", None)
    return jax.shard_map(
        step,
        mesh=mesh,
        in_specs=(seq, seq) + (rep,) * 3 + (own,) * 6,
        out_specs=(P("rep", None, None),) * 3 + (P("rep", "dp", None),) * 6,
        check_vma=False,
    )
```

```python
import functools

import jax
import jax.numpy as jnp
from jax import lax
from jax.experimental import pallas as pl
from jax.experimental.pallas import tpu as pltpu
from jax.sharding import PartitionSpec as P

F32, BF16 = jnp.float32, jnp.bfloat16
MESH = pl.DeviceIdType.MESH
NT = (((1,), (1,)), ((), ()))
CHUNK = 512
FORWARD_CHUNK = 1024
VMEM_LIMIT = 60 * 2**20
GATHER_QUARTERS = 16


def dot(a, b):
    return jnp.dot(a, b, preferred_element_type=F32)


def dot_nt(a, b):
    return lax.dot_general(a, b, NT, preferred_element_type=F32)


def scale_of(wide):
    return lax.rsqrt(jnp.mean(wide * wide, -1, keepdims=True) + 1e-6)


def forward_kernel(steps, x_ref, wg_ref, wu_ref, wd_ref, h_ref, a_ref, acc_ref):
    f = pl.program_id(0)

    @pl.when(f == 0)
    def _():
        wide = x_ref[...].astype(F32)
        a_ref[...] = (wide * scale_of(wide)).astype(BF16)
        acc_ref[...] = jnp.zeros_like(acc_ref)

    a = a_ref[...]
    gate, up = dot(a, wg_ref[0]), dot(a, wu_ref[0])
    act = (gate * jax.nn.sigmoid(gate) * up).astype(BF16)
    acc_ref[...] += dot(act, wd_ref[0])

    @pl.when(f == steps - 1)
    def _():
        h_ref[...] = x_ref[...] + acc_ref[...].astype(BF16)


def forward(x, wg, wu, wd, number):
    (tokens, d), ff = x.shape, wg.shape[2]
    steps = ff // FORWARD_CHUNK
    whole = pl.BlockSpec((tokens, d), lambda f: (0, 0))
    return pl.pallas_call(
        functools.partial(forward_kernel, steps),
        name="layer_forward",
        grid=(steps,),
        out_shape=jax.ShapeDtypeStruct(x.shape, BF16),
        in_specs=[whole]
        + [pl.BlockSpec((1, d, FORWARD_CHUNK), lambda f: (number, 0, f))] * 2
        + [pl.BlockSpec((1, FORWARD_CHUNK, d), lambda f: (number, f, 0))],
        out_specs=whole,
        scratch_shapes=[pltpu.VMEM((tokens, d), BF16), pltpu.VMEM((tokens, d), F32)],
        compiler_params=pltpu.CompilerParams(vmem_limit_bytes=VMEM_LIMIT),
        cost_estimate=pl.CostEstimate(flops=6 * tokens * d * ff, bytes_accessed=6 * d * ff, transcendentals=0),
    )(x, wg, wu, wd)


def wide_sum(*terms):
    total = terms[0].astype(F32)
    for t in terms[1:]:
        total = total + t.astype(F32)
    return total


def remote(src, dst, ssem, rsem, to):
    return pltpu.make_async_remote_copy(
        src_ref=src, dst_ref=dst, send_sem=ssem, recv_sem=rsem, device_id=to, device_id_type=MESH
    )


class Torus:
    def __init__(self, side):
        me = lax.axis_index("dp")
        self.side = side
        self.core, chip = lax.rem(me, 2), lax.div(me, 2)
        self.at = (lax.div(chip, side), lax.rem(chip, side))
        self.partner = self.device(*self.at, 1 - self.core)
        self.up = [lax.rem(p + 1, side) for p in self.at]
        self.down = [lax.rem(p + side - 1, side) for p in self.at]
        self.across = [lax.rem(p + 2, side) for p in self.at]
        self.far = [self.along(axis, self.across[axis]) for axis in (0, 1)]
        self.neighbour = [[self.along(axis, p[axis]) for p in (self.up, self.down)] for axis in (0, 1)]

    def device(self, x, y, c):
        return {"dp": (x * self.side + y) * 2 + c}

    def along(self, axis, p):
        return self.device(p, self.at[1], self.core) if axis == 0 else self.device(self.at[0], p, self.core)

    def next(self, axis, d):
        return self.up[axis] if d == 0 else self.down[axis]

    def greet(self, *more):
        barrier = pltpu.get_barrier_semaphore()
        for other in [self.partner, *self.neighbour[0], *self.neighbour[1], *more]:
            pl.semaphore_signal(barrier, inc=1, device_id=other, device_id_type=MESH)
        pl.semaphore_wait(barrier, 5 + len(more))


BOTH = [(st, d) for st in (0, 1) for d in (0, 1)]


class Pipe:
    def __init__(self, torus, count, lag, sources, sink, scratch):
        self.torus, self.count, self.lag, self.sources, self.sink = torus, count, lag, sources, sink
        self.S, self.r0, self.r1, self.r2, self.R, self.r3, self.r4, self.s0, self.v0, *rest = scratch
        (self.s1, self.v1, self.s2, self.v2, self.s3, self.v3, self.s4, self.v4) = rest
        self.half = self.S.shape[-1]

    @staticmethod
    def scratch(side, rows, width):
        half, dma = width // 2, pltpu.SemaphoreType.DMA
        return [
            pltpu.VMEM((6, 2, side, side, rows, half), BF16),
            pltpu.VMEM((4, side, side, rows, width), BF16),
            pltpu.VMEM((4, 2, 2, 2, rows, half), BF16),
            pltpu.VMEM((4, 2, 2, side, rows, half), BF16),
            pltpu.VMEM((6, 2, side, rows, half), BF16),
            pltpu.VMEM((4, 2, 2, rows, half // 2), BF16),
            pltpu.VMEM((4, 2, 2, rows, half), BF16),
            dma((4,)),
            dma((4,)),
        ] + [dma((4,))] * 8

    def s_at(self, st, slot, p, lo=0, n=4):
        return self.S.at[slot, st, p, pl.ds(lo, n)]

    def send0(self, view, par):
        return remote(view, self.r0.at[par], self.s0.at[par], self.v0.at[par], self.torus.partner)

    def any0(self, par):
        return self.send0(self.r0.at[par], par)

    def send1(self, st, d, slot, par):
        src, k = self.s_at(st, slot, self.torus.across[st], 2 * d, 2), (par, st, d)
        return remote(src, self.r1.at[k], self.s1.at[par], self.v1.at[par], self.torus.neighbour[st][d])

    def send2(self, st, d, slot, par):
        src, k = self.s_at(st, slot, self.torus.next(st, d)), (par, st, d)
        return remote(src, self.r2.at[k], self.s2.at[par], self.v2.at[par], self.torus.neighbour[st][d])

    def send3(self, st, d, slot, par):
        o, k, quarter = 1 - st, (par, st, d), self.half // 2
        src = self.R.at[slot, st, self.torus.across[o], :, pl.ds(d * quarter, quarter)]
        return remote(src, self.r3.at[k], self.s3.at[par], self.v3.at[par], self.torus.neighbour[o][d])

    def send4(self, st, d, slot, par):
        o, k = 1 - st, (par, st, d)
        src = self.R.at[slot, st, self.torus.next(o, d)]
        return remote(src, self.r4.at[k], self.s4.at[par], self.v4.at[par], self.torus.neighbour[o][d])

    def all(self, n, par):
        r, s, v = ((self.r1, self.s1, self.v1), (self.r2, self.s2, self.v2), (self.r3, self.s3, self.v3), (self.r4, self.s4, self.v4))[n - 1]
        return remote(r.at[par], r.at[par], s.at[par], v.at[par], self.torus.partner)

    def active(self, i):
        return jnp.logical_and(i >= 0, i < self.count)

    def within(self, i, source):
        return jnp.logical_and(i >= source[0], i < source[1])

    def sent(self, i, n, now):
        @pl.when(self.active(i))
        def _():
            self.all(n, now).wait_send()

    def turn(self, t):
        torus, S, R, half = self.torus, self.S, self.R, self.half
        now, before = lax.rem(t, 4), lax.rem(t + 2, 4)
        i = t - self.lag

        def slot6(i):
            return lax.rem(i, 6)

        @pl.when(self.active(i - 10))
        def _():
            slot = slot6(i - 10)
            self.all(4, before).wait_recv()
            for st in (0, 1):
                total = wide_sum(R[slot, st, torus.at[1 - st]], self.r4[before, st, 0], self.r4[before, st, 1])
                self.sink(i - 10, st, total.astype(BF16))

        self.sent(i - 12, 4, now)

        @pl.when(self.active(i - 8))
        def _():
            slot, quarter = slot6(i - 8), half // 2
            self.all(3, before).wait_recv()
            for st, d in BOTH:
                to, part = torus.next(1 - st, d), pl.ds(d * quarter, quarter)
                R[slot, st, to, :, part] = wide_sum(R[slot, st, to, :, part], self.r3[before, st, d]).astype(BF16)
            for st, d in BOTH:
                self.send4(st, d, slot, now).start()

        self.sent(i - 10, 3, now)

        @pl.when(self.active(i - 6))
        def _():
            slot = slot6(i - 6)
            self.all(2, before).wait_recv()
            for st in (0, 1):
                for k in range(torus.side):
                    R[slot, st, k] = wide_sum(S[slot, st, torus.at[st], k], self.r2[before, st, 0, k], self.r2[before, st, 1, k]).astype(BF16)
            for st, d in BOTH:
                self.send3(st, d, slot, now).start()

        self.sent(i - 8, 2, now)

        @pl.when(self.active(i - 4))
        def _():
            slot = slot6(i - 4)
            self.all(1, before).wait_recv()
            for st, d in BOTH:
                to = torus.next(st, d)
                for k in (0, 1):
                    S[slot, st, to, 2 * d + k] = wide_sum(S[slot, st, to, 2 * d + k], self.r1[before, st, d, k]).astype(BF16)
            for st, d in BOTH:
                self.send2(st, d, slot, now).start()

        self.sent(i - 6, 1, now)

        @pl.when(self.active(i - 2))
        def _():
            self.any0(before).wait_recv()
            slot = slot6(i - 2)
            for source in self.sources:

                @pl.when(self.within(i - 2, source))
                def _(source=source):
                    def add(k, carry):
                        kx, ky = lax.div(k, torus.side), lax.rem(k, torus.side)
                        mine = source[2](i - 2, torus.core).at[kx, ky][...]
                        both = wide_sum(mine, self.r0[before, kx, ky]).astype(BF16)
                        S[slot, 0, kx, ky], S[slot, 1, ky, kx] = both[:, :half], both[:, half:]
                        return carry

                    lax.fori_loop(0, torus.side**2, add, 0, unroll=4)

            for st, d in BOTH:
                self.send1(st, d, slot, now).start()

        @pl.when(self.active(i - 2))
        def _():
            self.any0(before).wait_send()

        for source in self.sources:

            @pl.when(self.within(i, source))
            def _(source=source):
                self.send0(source[2](i, 1 - torus.core), now).start()


def gradient_kernel(
    side, ff, chunk, count, x_ref, h_ref, dy_ref, wg_hbm, wu_hbm, wd_hbm, out_ref, factor_ref,
    a_ref, at_ref, dy_now, dg_acc, du_acc, w_buf, w_sem, C, D, sqs, sqr, qs, qv, *pipes,
):
    torus = Torus(side)
    steps = ff // chunk
    rows, d = out_ref.shape[1], x_ref.shape[1]
    torus.greet(*torus.far)

    def set_input(ref):
        wide = ref[...].astype(F32)
        a = (wide * scale_of(wide)).astype(BF16)
        a_ref[...] = a
        at_ref[...] = a.T

    def loads(t, slot):
        number, f = 1 - lax.div(t, steps), lax.rem(t, steps)
        part = pl.ds(pl.multiple_of(f * chunk, chunk), chunk)
        return [
            pltpu.make_async_copy(wg_hbm.at[number, :, part], w_buf.at[slot, 0], w_sem.at[slot, 0]),
            pltpu.make_async_copy(wu_hbm.at[number, :, part], w_buf.at[slot, 1], w_sem.at[slot, 1]),
            pltpu.make_async_copy(wd_hbm.at[number, part, :], w_buf.at[slot, 2], w_sem.at[slot, 2]),
        ]

    for copy in loads(0, 0):
        copy.start()
    dy_now[...] = dy_ref[...]
    sqs[0] = jnp.zeros(sqs.shape[1:], F32)
    dg_acc[...] = jnp.zeros_like(dg_acc)
    du_acc[...] = jnp.zeros_like(du_acc)
    set_input(h_ref)

    def compute(t, inner):
        slot, c_slot = lax.rem(t, 2), lax.rem(t, C.shape[0])
        f = lax.rem(t, steps)
        a, dy = a_ref[...], dy_now[...]
        wg, wu, wd = (w_buf[slot, k] for k in range(3))
        gate, up = dot(a, wg), dot(a, wu)
        dact = dot_nt(dy, wd).astype(BF16).astype(F32)
        sig = jax.nn.sigmoid(gate)
        silu = gate * sig
        act = (silu * up).astype(BF16)
        dup = (dact * silu).astype(BF16)
        dgate = (dact * up * (sig + silu * (1.0 - sig))).astype(BF16)
        if inner:
            dg_acc[...] += dot_nt(dgate, wg)
            du_acc[...] += dot_nt(dup, wu)
        at = at_ref[...]
        for k, g in enumerate((dgate, dup)):
            blocks = dot(at, g).astype(BF16).reshape(side, side, 2, rows, chunk)
            for c in range(2):
                C[c_slot, c, :, :, :, k * chunk : (k + 1) * chunk] = blocks[:, :, c]
        dwd = lax.dot_general(act, dy, (((0,), (0,)), ((), ())), preferred_element_type=F32).astype(BF16)
        pieces = ff // d
        for b in range(2):
            for k in range(pieces):
                row = (b * pieces + k) * rows
                D[1 if inner else 0, b, lax.div(f, side), lax.rem(f, side), :, k * d : (k + 1) * d] = dwd[row : row + rows]

    def squares(total):
        wide = total.astype(F32)
        sqs[0] += jnp.sum(jnp.sum((wide * wide).reshape(2, 8, -1, 128), axis=2), axis=0)

    def d_view(layer, first, width):
        def view(i, c):
            return D.at[layer, c, :, :, :, pl.ds(pl.multiple_of((i - first) * width, width), width)]

        return view

    def c_view(i, c):
        return C.at[lax.rem(i, C.shape[0]), c]

    def sink_main(i, st, total):
        squares(total)

        @pl.when(i < 2 * steps)
        def _():
            where = pl.ds(pl.multiple_of(lax.rem(i, steps) * chunk, chunk), chunk)
            out_ref[3 * lax.div(i, steps) + st, :, where] = total

        @pl.when(i >= 2 * steps)
        def _():
            where = pl.ds(pl.multiple_of((i - 2 * steps) * 2 * chunk + st * chunk, chunk), chunk)
            out_ref[5, :, where] = total

    def sink_down(i, st, total):
        squares(total)
        width = chunk // 2
        out_ref[2, :, pl.ds(pl.multiple_of(i * chunk + st * width, width), width)] = total

    tail = steps // 2
    n = len(pipes) // 2
    main = Pipe(
        torus, 2 * steps + tail, 1,
        [(0, 2 * steps, c_view), (2 * steps, 2 * steps + tail, d_view(0, 2 * steps, 2 * chunk))], sink_main, pipes[:n],
    )
    down = Pipe(torus, steps, steps + 1, [(0, steps, d_view(1, 0, chunk))], sink_down, pipes[n:])

    def body(t, carry):
        @pl.when(t == steps)
        def _():
            set_input(x_ref)

        main.turn(t)
        down.turn(t)

        @pl.when(t < 2 * steps)
        def _():
            @pl.when(t + 1 < 2 * steps)
            def _():
                for copy in loads(t + 1, lax.rem(t + 1, 2)):
                    copy.start()

            for copy in loads(t, lax.rem(t, 2)):
                copy.wait()

        @pl.when(t < steps)
        def _():
            compute(t, True)

        @pl.when(t == steps - 1)
        def _():
            da = (dg_acc[...].astype(BF16).astype(F32) + du_acc[...].astype(BF16).astype(F32)).astype(BF16).astype(F32)
            wide = h_ref[...].astype(F32)
            s = scale_of(wide)
            along = jnp.mean(da * wide, -1, keepdims=True)
            dy_now[...] = dy_ref[...] + (da * s - wide * (s * s * s * along)).astype(BF16)

        @pl.when(jnp.logical_and(t >= steps, t < 2 * steps))
        def _():
            compute(t, False)

        return carry

    lax.fori_loop(0, 2 * steps + tail + 13, body, 0)

    rounds = [[torus.partner]] + [torus.neighbour[axis] + [torus.far[axis]] for axis in (0, 1)]
    for k, others in enumerate(rounds):
        swaps = [remote(sqs.at[k], sqr.at[k, j], qs.at[k, j], qv.at[k, j], other) for j, other in enumerate(others)]
        for swap in swaps:
            swap.start()
        for swap in swaps:
            swap.wait()
        total = sqs[k]
        for j in range(len(others)):
            total = total + sqr[k, j]
        sqs[k + 1] = total
    total = jnp.broadcast_to(jnp.sum(sqs[len(rounds)], keepdims=True), factor_ref.shape)
    factor_ref[...] = jnp.minimum(1.0, 0.5 * lax.rsqrt(total / count + 1e-30))


def summed_gradients(x, h, dy, w, n):
    (tokens, d), ff = x.shape, w[0].shape[2]
    side = round((n // 2) ** 0.5)
    assert side == 4 and n == 2 * side * side and w[0].shape[0] == 2
    rows, chunk = d // n, CHUNK
    assert 2 * ff // n == chunk
    dma, vmem = pltpu.SemaphoreType.DMA, pl.BlockSpec(memory_space=pltpu.VMEM)
    return pl.pallas_call(
        functools.partial(gradient_kernel, side, ff, chunk, sum(t.size for t in w)),
        name="summed_gradients",
        out_shape=(jax.ShapeDtypeStruct((6, rows, ff), BF16), jax.ShapeDtypeStruct((8, 128), F32)),
        in_specs=[vmem] * 3 + [pl.BlockSpec(memory_space=pl.ANY)] * 3,
        out_specs=(vmem, vmem),
        scratch_shapes=[
            pltpu.VMEM((tokens, d), BF16),
            pltpu.VMEM((d, tokens), BF16),
            pltpu.VMEM((tokens, d), BF16),
            pltpu.VMEM((tokens, d), F32),
            pltpu.VMEM((tokens, d), F32),
            pltpu.VMEM((2, 3, d, chunk), BF16),
            dma((2, 3)),
            pltpu.VMEM((3, 2, side, side, rows, 2 * chunk), BF16),
            pltpu.VMEM((2, 2, side, side, rows, ff), BF16),
            pltpu.VMEM((4, 8, 128), F32),
            pltpu.VMEM((3, 3, 8, 128), F32),
            dma((3, 3)),
            dma((3, 3)),
        ]
        + Pipe.scratch(side, rows, 2 * chunk)
        + Pipe.scratch(side, rows, chunk),
        compiler_params=pltpu.CompilerParams(collective_id=1, has_side_effects=True, vmem_limit_bytes=67043328),
        cost_estimate=pl.CostEstimate(flops=28 * tokens * d * ff, bytes_accessed=12 * d * ff, transcendentals=0),
    )(x, h, dy, *w)


def gather_kernel(
    side, own_gate, own_up, own_down, out_gate, out_up, out_down, own_sem, sa, va, sb, vb, sc, vc, sd, vd, se, ve
):
    torus = Torus(side)
    outs, owns = (out_gate, out_up, out_down), (own_gate, own_up, own_down)
    x, y = torus.at
    core = torus.core
    quarter = [ref.shape[-1] // GATHER_QUARTERS for ref in outs[:2]] + [out_down.shape[-2] // GATHER_QUARTERS]
    per_layer = GATHER_QUARTERS // 4
    layers = out_gate.shape[0]
    per_kind = layers * per_layer
    count = 3 * per_kind

    own_copies = [
        pltpu.make_async_copy(own, out.at[:, x, y, core], own_sem.at[k]) for k, (own, out) in enumerate(zip(owns, outs))
    ]
    for copy in own_copies:
        copy.start()
    torus.greet()
    for copy in own_copies:
        copy.wait()

    def part(kind, i, first, n):
        where = pl.ds(
            pl.multiple_of((lax.rem(i, per_layer) * 4 + first) * quarter[kind], quarter[kind]), n * quarter[kind]
        )
        return (slice(None), where) if kind < 2 else (where, slice(None))

    def layer_of(kind, i):
        return lax.div(i - kind * per_kind, per_layer)

    def place(kind, i, st, p, q, first, n):
        where = (p, q) if st == 0 else (q, p)
        return outs[kind].at[(layer_of(kind, i), *where, core, *part(kind, i, first, n))]

    ALL = slice(None)

    def send_a(kind, i, st, d, par):
        dst = place(kind, i, st, torus.at[st], torus.at[1 - st], 2 * st, 2)
        src = owns[kind].at[(layer_of(kind, i), *part(kind, i, 2 * st, 2))]
        k = (par, st, d)
        return remote(src, dst, sa.at[k], va.at[k], torus.neighbour[1 - st][d])

    def send_b(kind, i, st, d, par):
        o = 1 - st
        ref, k = place(kind, i, st, torus.at[st], torus.next(o, 1 - d), 2 * st + d, 1), (par, st, d)
        return remote(ref, ref, sb.at[k], vb.at[k], torus.neighbour[o][d])

    def send_c(kind, i, st, d, par):
        ref, k = place(kind, i, st, torus.at[st], ALL, 2 * st, 2), (par, st, d)
        return remote(ref, ref, sc.at[k], vc.at[k], torus.neighbour[st][d])

    def send_d(kind, i, st, d, par):
        ref, k = place(kind, i, st, torus.next(st, 1 - d), pl.ds(2 * d, 2), 2 * st, 2), (par, st, d)
        return remote(ref, ref, sd.at[k], vd.at[k], torus.neighbour[st][d])

    def send_e(kind, i, par):
        ref = outs[kind].at[(layer_of(kind, i), ALL, ALL, core, *part(kind, i, 0, 4))]
        return remote(ref, ref, se.at[par], ve.at[par], torus.partner)

    def active(i):
        return jnp.logical_and(i >= 0, i < count)

    sends = [send_a, send_b, send_c, send_d]

    def body(t, carry):
        now, before = lax.rem(t, 4), lax.rem(t + 2, 4)

        @pl.when(active(t - 10))
        def _():
            send_e(0, 0, before).wait_recv()

        @pl.when(active(t - 12))
        def _():
            send_e(0, 0, now).wait_send()

        @pl.when(active(t - 8))
        def _():
            for st, d in BOTH:
                send_d(0, 0, st, d, before).wait_recv()
            for kind in range(3):

                @pl.when(lax.div(t - 8, per_kind) == kind)
                def _(kind=kind):
                    send_e(kind, t - 8, now).start()

        for s in (3, 2, 1, 0):

            @pl.when(active(t - 2 * s - 4))
            def _(s=s):
                for st, d in BOTH:
                    sends[s](0, 0, st, d, now).wait_send()

            @pl.when(active(t - 2 * s))
            def _(s=s):
                if s:
                    for st, d in BOTH:
                        sends[s - 1](0, 0, st, d, before).wait_recv()
                for kind in range(3):

                    @pl.when(lax.div(t - 2 * s, per_kind) == kind)
                    def _(kind=kind):
                        for st, d in BOTH:
                            sends[s](kind, t - 2 * s, st, d, now).start()

        return carry

    lax.fori_loop(0, count + 12, body, 0)


def gathered(blocks, n):
    side = round((n // 2) ** 0.5)
    assert side == 4 and n == 2 * side * side
    dma = pltpu.SemaphoreType.DMA
    whole = pl.pallas_call(
        functools.partial(gather_kernel, side),
        name="gather_weights",
        out_shape=[jax.ShapeDtypeStruct((b.shape[0], side, side, 2, *b.shape[1:]), b.dtype) for b in blocks],
        in_specs=[pl.BlockSpec(memory_space=pltpu.VMEM)] * 3,
        out_specs=[pl.BlockSpec(memory_space=pl.ANY)] * 3,
        scratch_shapes=[dma((3,))] + [dma((4, 2, 2))] * 8 + [dma((4,))] * 2,
        compiler_params=pltpu.CompilerParams(collective_id=2, has_side_effects=True, vmem_limit_bytes=16 * 2**20),
        cost_estimate=pl.CostEstimate(flops=10**8, bytes_accessed=10**8, transcendentals=0),
    )(*blocks)
    return [t.reshape(t.shape[0], -1, t.shape[-1]) for t in whole]


def adamw(w, m, v, g):
    m = 0.9 * m + 0.1 * g
    v = 0.95 * v + 0.05 * g * g
    step = m * lax.rsqrt(v + 1e-8) + 0.1 * w
    return (w - 0.02 * step).astype(jnp.bfloat16), m, v


def solution(mesh):
    n = mesh.shape["dp"]

    def step(x, dy, *arrays):
        w, m, v = (arrays[i : i + 3] for i in (0, 3, 6))
        x, dy = x[0], dy[0]
        me = lax.axis_index("dp")
        h = forward(x, *w, 0)
        summed, factor = summed_gradients(x, h, dy, w, n)
        factor = factor[0, 0]
        outs = []
        for k in range(3):
            rows = m[k].shape[1]
            g = jnp.stack([summed[3 + k], summed[k]])
            if k == 2:
                g = g.reshape(2, g.shape[1], -1, m[k].shape[2]).swapaxes(1, 2).reshape(m[k].shape)
            own = lax.dynamic_slice_in_dim(w[k], me * rows, rows, 1)
            outs.append(adamw(own.astype(F32), m[k], v[k], g.astype(F32) * factor))
        new = gathered([one[0] for one in outs], n)
        return (*new, *(one[1] for one in outs), *(one[2] for one in outs))

    seq, rep, own = P(("rep", "dp"), None, None), P(None, None, None), P(None, "dp", None)
    return jax.shard_map(
        step,
        mesh=mesh,
        in_specs=(seq, seq) + (rep,) * 3 + (own,) * 6,
        out_specs=(P("rep", None, None),) * 3 + (P("rep", "dp", None),) * 6,
        check_vma=False,
    )
```
